32 devices in a mesh: batch: 1 (over z), cols: 4 (over y), rows: 8 (over x, core).
Axes of the slice: x: 4, y: 4, z: 1, core: 2. Of those that a mesh axis runs over, the one named last changes fastest.
The devices are a block of a 4x4x8 slice.
Arguments:
- frames: bfloat16 [12, 2, 192, 96, 16], P(None, 'batch', 'rows', 'cols')
- w_x: bfloat16 [3, 3, 16, 512], replicated
- w_h: bfloat16 [3, 3, 128, 512], replicated
- gate_bias: float32 [512], replicated
- h_init: bfloat16 [2, 192, 96, 128], P('batch', 'rows', 'cols')
- c_init: float32 [2, 192, 96, 128], P('batch', 'rows', 'cols')
Outputs:
- output 1: bfloat16 [12, 2, 192, 96, 128], P(None, 'batch', 'rows', 'cols')
- output 2: float32 [2, 192, 96, 128], P('batch', 'rows', 'cols')
All inputs are finite; a program needn't handle non-finite values.
Results may differ from the reference program's by a relative error of at most 0.00230549.
Values are sent between devices in bfloat16 or wider.
A program may use at most 768 MiB of HBM per device.

```python
import jax
import jax.numpy as jnp
from jax import lax

STEPS = 12
SAMPLES = 2
GRID_HEIGHT = 192
GRID_WIDTH = 96
IN_CHANNELS = 16
HIDDEN = 128
BAND_ROWS = 8


def setup_inputs(seed: int = 0, part: int = 0) -> dict:
    root_key = jax.random.key(seed)
    shared_key, local_root = jax.random.split(root_key)
    local_key = jax.random.fold_in(local_root, part)
    key_wx, key_wh, key_bias = jax.random.split(shared_key, 3)
    key_frames, key_hidden, key_cell = jax.random.split(local_key, 3)
    gate_width = 4 * HIDDEN
    frames = jax.random.normal(key_frames, (STEPS, SAMPLES, GRID_HEIGHT, GRID_WIDTH, IN_CHANNELS), jnp.float32)
    w_x = jax.random.normal(key_wx, (3, 3, IN_CHANNELS, gate_width), jnp.float32) * (0.8 * (9 * IN_CHANNELS) ** -0.5)
    w_h = jax.random.normal(key_wh, (3, 3, HIDDEN, gate_width), jnp.float32) * (1.5 * (9 * HIDDEN) ** -0.5)
    forget_shift = jnp.concatenate([jnp.zeros((HIDDEN,), jnp.float32), jnp.ones((HIDDEN,), jnp.float32), jnp.zeros((2 * HIDDEN,), jnp.float32)])
    gate_bias = 0.5 * jax.random.normal(key_bias, (gate_width,), jnp.float32) + forget_shift
    h_init = 0.5 * jax.random.normal(key_hidden, (SAMPLES, GRID_HEIGHT, GRID_WIDTH, HIDDEN), jnp.float32)
    c_init = jax.random.normal(key_cell, (SAMPLES, GRID_HEIGHT, GRID_WIDTH, HIDDEN), jnp.float32)
    return {"frames": frames.astype(jnp.bfloat16), "w_x": w_x.astype(jnp.bfloat16), "w_h": w_h.astype(jnp.bfloat16), "gate_bias": gate_bias, "h_init": h_init.astype(jnp.bfloat16), "c_init": c_init}


def conv_taps(padded, weights, out_rows, out_cols):
    tap_list = [padded[:, row_off:row_off + out_rows, col_off:col_off + out_cols, :] for row_off in range(3) for col_off in range(3)]
    patches = jnp.concatenate(tap_list, axis=-1)
    flat_patches = patches.reshape(-1, patches.shape[-1])
    flat_weights = weights.reshape(-1, weights.shape[-1])
    product = jnp.dot(flat_patches, flat_weights, preferred_element_type=jnp.float32)
    return product.reshape(padded.shape[0], out_rows, out_cols, -1)


def lstm_cell(gate_sum, cell_prev):
    hidden_width = cell_prev.shape[-1]
    in_gate = jax.nn.sigmoid(gate_sum[..., :hidden_width])
    forget_gate = jax.nn.sigmoid(gate_sum[..., hidden_width:2 * hidden_width])
    out_gate = jax.nn.sigmoid(gate_sum[..., 2 * hidden_width:3 * hidden_width])
    cand_gate = jnp.tanh(gate_sum[..., 3 * hidden_width:])
    cell_next = forget_gate * cell_prev + in_gate * cand_gate
    hidden_next = (out_gate * jnp.tanh(cell_next)).astype(jnp.bfloat16)
    return hidden_next, cell_next


def reference(frames, w_x, w_h, gate_bias, h_init, c_init):
    num_bands = GRID_HEIGHT // BAND_ROWS
    pad_cfg = ((0, 0), (1, 1), (1, 1), (0, 0))

    def step_fn(state_pair, frame_t):
        hidden, cell_state = state_pair
        frame_pad = jnp.pad(frame_t, pad_cfg)
        hidden_pad = jnp.pad(hidden, pad_cfg)

        def band_update(band_index):
            row_start = band_index * BAND_ROWS
            frame_band = lax.dynamic_slice_in_dim(frame_pad, row_start, BAND_ROWS + 2, axis=1)
            hidden_band = lax.dynamic_slice_in_dim(hidden_pad, row_start, BAND_ROWS + 2, axis=1)
            cell_band = lax.dynamic_slice_in_dim(cell_state, row_start, BAND_ROWS, axis=1)
            gate_sum = conv_taps(frame_band, w_x, BAND_ROWS, GRID_WIDTH) + conv_taps(hidden_band, w_h, BAND_ROWS, GRID_WIDTH) + gate_bias
            return lstm_cell(gate_sum, cell_band)

        band_hidden, band_cell = lax.map(band_update, jnp.arange(num_bands))
        hidden_next = jnp.moveaxis(band_hidden, 0, 1).reshape(SAMPLES, GRID_HEIGHT, GRID_WIDTH, HIDDEN)
        cell_next = jnp.moveaxis(band_cell, 0, 1).reshape(SAMPLES, GRID_HEIGHT, GRID_WIDTH, HIDDEN)
        return (hidden_next, cell_next), hidden_next

    final_pair, all_hidden = lax.scan(step_fn, (h_init, c_init), frames)
    return all_hidden, final_pair[1]
```

```python
import jax
import jax.numpy as jnp
from jax import lax
from jax.experimental import pallas as pl
from jax.experimental.pallas import tpu as pltpu
from jax.sharding import PartitionSpec as P

BLOCK = 3
COL0 = 8
DIRS = ((-1, 0), (1, 0), (0, -1), (0, 1), (-1, -1), (-1, 1), (1, -1), (1, 1))
MESH = pl.DeviceIdType.MESH
F32 = jnp.float32
BF16 = jnp.bfloat16


def opposite(k):
    return DIRS.index((-DIRS[k][0], -DIRS[k][1]))


def make_kernel(steps, seqs, rows, cols, chan, hid, row_count, col_count):
    nblock = steps // BLOCK
    pitch = cols + 16
    hrows = rows + 2 * BLOCK + 6
    ring = BLOCK - 1
    xrow0 = 8
    nstrip = 2 * ring
    gates = 4 * hid
    kdim = 9 * hid + 3 * 128
    strip_cols = tuple(range(-ring, 0)) + tuple(range(cols, cols + ring))
    third = rows // 3

    def chunk_list(ext):
        own = [c for c in range(nstrip) if -ext <= strip_cols[c] < cols + ext]
        return (
            (-ext, third + ext, ()),
            (third, third, tuple(own)),
            (2 * third, third + ext, ()),
        )

    def kernel(frames, wx_ref, wh_hbm, bias_ref, hinit, cinit, hout, cout, *scratch):
        (hb0a, hb1a, hb2a, hb0b, hb1b, hb2b, xga, xgb, cma, cmb, csa, csb, xt, fbuf, wall,
         lhs0, lhs1, lhs2, gs0, gs1, gs2, ob, hin, sh, sc, sch, scc, rh, rc, rch, rcc, tmp, smask,
         lsem, osem, ssem, rsem, xssem, xrsem) = scratch
        hbs = ((hb0a, hb1a, hb2a), (hb0b, hb1b, hb2b))
        xgs = (xga, xgb)
        cms = (cma, cmb)
        css = (csa, csb)
        lhss = (lhs0, lhs1, lhs2)
        gss = (gs0, gs1, gs2)

        ri = lax.axis_index("rows")
        ci = lax.axis_index("cols")

        def exists(k):
            dr, dc = DIRS[k]
            conds = []
            if dr < 0:
                conds.append(ri > 0)
            if dr > 0:
                conds.append(ri < row_count - 1)
            if dc < 0:
                conds.append(ci > 0)
            if dc > 0:
                conds.append(ci < col_count - 1)
            out = conds[0]
            for extra in conds[1:]:
                out = jnp.logical_and(out, extra)
            return out

        def dev(k):
            return {"rows": ri + DIRS[k][0], "cols": ci + DIRS[k][1]}

        def h_addr(r, c):
            return (r + BLOCK) * pitch + COL0 + c

        def x_addr(r, c):
            return (r + ring) * pitch + COL0 + c

        cp_h = pltpu.make_async_copy(hinit, hin, lsem.at[0])
        cp_f = pltpu.make_async_copy(frames, fbuf, lsem.at[1])
        cp_w = pltpu.make_async_copy(wh_hbm, wall.at[pl.ds(0, 9 * hid), :], lsem.at[2])
        cp_c = [pltpu.make_async_copy(cinit.at[s], cms[s].at[pl.ds(ring * cols, rows * cols), :], lsem.at[3 + s]) for s in range(seqs)]
        cp_h.start()
        for s in range(seqs):
            cp_c[s].start()
        cp_f.start()
        cp_w.start()

        barrier = pltpu.get_barrier_semaphore()
        rh[...] = jnp.zeros_like(rh)
        rc[...] = jnp.zeros_like(rc)
        rch[...] = jnp.zeros_like(rch)
        rcc[...] = jnp.zeros_like(rcc)

        def zero_x(i, _):
            xt[i] = jnp.zeros(xt.shape[1:], F32)
            return 0

        lax.fori_loop(0, steps * seqs, zero_x, 0)
        for k in range(8):
            @pl.when(exists(k))
            def _():
                pl.semaphore_signal(barrier, 1, device_id=dev(k), device_id_type=MESH)
        for s in range(seqs):
            for q in range(3):
                hbs[s][q][...] = jnp.zeros_like(hbs[s][q])
            css[s][...] = jnp.zeros_like(css[s])
            cms[s][pl.ds(0, ring * cols), :] = jnp.zeros((ring * cols, hid), F32)
            cms[s][pl.ds((rows + ring) * cols, ring * cols), :] = jnp.zeros((ring * cols, hid), F32)
            xgs[s][...] = jnp.zeros_like(xgs[s])

        top_ok = jnp.where(ri > 0, 1.0, 0.0).astype(F32)
        bot_ok = jnp.where(ri < row_count - 1, 1.0, 0.0).astype(F32)
        left_ok = jnp.where(ci > 0, 1.0, 0.0).astype(F32)
        right_ok = jnp.where(ci < col_count - 1, 1.0, 0.0).astype(F32)
        srow = lax.broadcasted_iota(jnp.int32, (32, hid), 0)
        rmask = jnp.where(srow < ring, top_ok, jnp.where(srow >= rows + ring, bot_ok, 1.0))
        smask[0] = rmask * left_ok
        smask[1] = rmask * right_ok

        n_row = jnp.where(ri > 0, 1, 0) + jnp.where(ri < row_count - 1, 1, 0)
        n_col = jnp.where(ci > 0, 1, 0) + jnp.where(ci < col_count - 1, 1, 0)
        pl.semaphore_wait(barrier, (n_row + 1) * (n_col + 1) - 1)

        def msg_copies(s, k, par):
            if k < 4:
                pairs = ((sh.at[s, k], rh.at[par, s, k]), (sc.at[s, k], rc.at[par, s, k]))
            else:
                pairs = ((sch.at[s, k - 4], rch.at[par, s, k - 4]), (scc.at[s, k - 4], rcc.at[par, s, k - 4]))
            return [
                pltpu.make_async_remote_copy(src_ref=a, dst_ref=b, send_sem=ssem.at[s, k, n], recv_sem=rsem.at[par, s, k, n], device_id=dev(k), device_id_type=MESH)
                for n, (a, b) in enumerate(pairs)
            ]

        def pack(s):
            hb = hbs[s][0]
            cm = cms[s]
            for k in range(8):
                dr, dc = DIRS[k]
                r0 = 0 if dr < 0 else rows - BLOCK
                rc0 = 0 if dr < 0 else rows - ring
                c0 = 0 if dc < 0 else cols - BLOCK
                cc0 = 0 if dc < 0 else cols - ring
                if dc == 0:
                    v = jnp.concatenate([hb[pl.ds(h_addr(r0 + i, 0), cols), :] for i in range(BLOCK)], axis=0)
                    sh[s, k, pl.ds(0, BLOCK * cols), :] = v.astype(BF16)
                    sc[s, k] = cm[pl.ds((rc0 + ring) * cols, ring * cols), :]
                elif dr == 0:
                    v = jnp.concatenate([hb[pl.ds(h_addr(0, c0 + j), rows, stride=pitch), :] for j in range(BLOCK)], axis=0)
                    sh[s, k, pl.ds(0, BLOCK * rows), :] = v.astype(BF16)
                    for j in range(ring):
                        sc[s, k, pl.ds(j * rows, rows), :] = cm[pl.ds(ring * cols + cc0 + j, rows, stride=cols), :]
                else:
                    for i in range(BLOCK):
                        tmp[pl.ds(i * BLOCK, BLOCK), :] = hb[pl.ds(h_addr(r0 + i, c0), BLOCK), :]
                    sch[s, k - 4] = tmp[pl.ds(0, 16), :].astype(BF16)
                    for j in range(ring):
                        scc[s, k - 4, pl.ds(j * ring, ring), :] = cm[pl.ds((rc0 + ring) * cols + cc0 + j, ring, stride=cols), :]

        def unpack(s, par):
            hb = hbs[s][0]
            cm = cms[s]
            cs = css[s]
            for k in range(8):
                dr, dc = DIRS[k]
                o = opposite(k)
                r0 = -BLOCK if dr < 0 else rows
                c0 = -BLOCK if dc < 0 else cols
                st0 = 0 if dc < 0 else ring
                q0 = 0 if dr < 0 else rows + ring
                if dc == 0:
                    v = rh[par, s, o, pl.ds(0, BLOCK * cols), :].astype(F32)
                    for i in range(BLOCK):
                        hb[pl.ds(h_addr(r0 + i, 0), cols), :] = v[i * cols:(i + 1) * cols]
                    cm[pl.ds(q0 * cols, ring * cols), :] = rc[par, s, o]
                elif dr == 0:
                    v = rh[par, s, o, pl.ds(0, BLOCK * rows), :].astype(F32)
                    for j in range(BLOCK):
                        hb[pl.ds(h_addr(0, c0 + j), rows, stride=pitch), :] = v[j * rows:(j + 1) * rows]
                    for j in range(ring):
                        cs[pl.ds((st0 + j) * 32 + ring, rows), :] = rc[par, s, o, pl.ds(j * rows, rows), :]
                else:
                    tmp[pl.ds(0, 16), :] = rch[par, s, o - 4].astype(F32)
                    for i in range(BLOCK):
                        hb[pl.ds(h_addr(r0 + i, c0), BLOCK), :] = tmp[pl.ds(i * BLOCK, BLOCK), :]
                    for j in range(ring):
                        cs[pl.ds((st0 + j) * 32 + q0, ring), :] = rcc[par, s, o - 4, pl.ds(j * ring, ring), :]

        def send(s, par):
            for k in range(8):
                @pl.when(exists(k))
                def _():
                    for cp in msg_copies(s, k, par):
                        cp.start()

        def wait_send(s):
            for k in range(8):
                @pl.when(exists(k))
                def _():
                    for cp in msg_copies(s, k, 0):
                        cp.wait_send()

        def wait_recv(s, par):
            for k in range(8):
                @pl.when(exists(k))
                def _():
                    for cp in msg_copies(s, opposite(k), par):
                        cp.wait_recv()

        own_lane = xrow0 * chan
        row_lanes = rows * chan

        def x_copy(t, k):
            dr, dc = DIRS[k]
            if dr == 0:
                lanes_s, lanes_d, lane_n = own_lane, own_lane, row_lanes
            else:
                lane_n = 8 * chan
                lanes_s = own_lane if dr < 0 else own_lane + row_lanes - lane_n
                lanes_d = own_lane + row_lanes if dr < 0 else 0
            if dc == 0:
                sub_s, sub_d, sub_n = COL0, COL0, cols
            else:
                sub_n = 8
                sub_s = COL0 if dc < 0 else COL0 + cols - 8
                sub_d = COL0 + cols if dc < 0 else 0
            return pltpu.make_async_remote_copy(
                src_ref=xt.at[pl.ds(t * seqs, seqs), pl.ds(sub_s, sub_n), pl.ds(lanes_s, lane_n)],
                dst_ref=xt.at[pl.ds(t * seqs, seqs), pl.ds(sub_d, sub_n), pl.ds(lanes_d, lane_n)],
                send_sem=xssem.at[t, k], recv_sem=xrsem.at[t, k], device_id=dev(k), device_id_type=MESH)

        cp_h.wait()
        for s in range(seqs):
            for r in range(0, rows, 2):
                v = hin[s, pl.ds(r * cols, 2 * cols), :].astype(F32)
                for i in range(2):
                    hbs[s][0][pl.ds(h_addr(r + i, 0), cols), :] = v[i * cols:(i + 1) * cols]
            cp_c[s].wait()
            pack(s)
            send(s, 0)

        eye = (lax.broadcasted_iota(jnp.int32, (cols, cols), 0) == lax.broadcasted_iota(jnp.int32, (cols, cols), 1)).astype(F32).astype(BF16)
        cp_f.wait()

        def prep_x(t, _):
            for s in range(seqs):
                xt[t * seqs + s, pl.ds(COL0, cols), pl.ds(own_lane, row_lanes)] = lax.dot_general(
                    eye, fbuf[t * seqs + s], (((1,), (1,)), ((), ())), preferred_element_type=F32)
            for k in range(8):
                @pl.when(exists(k))
                def _():
                    x_copy(t, k).start()
            return 0

        lax.fori_loop(0, steps, prep_x, 0)

        cp_w.wait()
        wall[pl.ds(9 * hid, 3 * 128), :] = jnp.zeros((3 * 128, gates), BF16)
        for dc in range(3):
            for dr in range(3):
                wall[pl.ds(9 * hid + dc * 128 + dr * chan, chan), :] = wx_ref[dr, dc]

        lane = lax.broadcasted_iota(jnp.int32, (pitch, 128), 1)

        def build_xg(s, t, ext):
            xg = xgs[s]
            for r in range(-ext, rows + ext):
                start = r - 1 + xrow0
                g, off = divmod(start, 8)
                v = xt[t * seqs + s, :, pl.ds(g * 128, 128)]
                if off:
                    v = pltpu.roll(v, 128 - chan * off, 1)
                    if off > 5:
                        w = pltpu.roll(xt[t * seqs + s, :, pl.ds((g + 1) * 128, 128)], 128 - chan * off, 1)
                        v = jnp.where(lane < 128 - chan * off, v, w)
                xg[pl.ds(x_addr(r, -COL0), pitch), :] = v

        def build_lhs(s, j, ch):
            hb = hbs[s][j]
            xg = xgs[s]
            r0, nr, strips = chunk_list(BLOCK - 1 - j)[ch]
            lhs = lhss[ch]
            base = 32 * len(strips)
            for tap in range(12):
                for n, k in enumerate(strips):
                    if tap < 9:
                        dr, dc = tap // 3 - 1, tap % 3 - 1
                        v = hb[pl.ds(h_addr(-ring + dr, strip_cols[k] + dc), 32, stride=pitch), :]
                    else:
                        v = xg[pl.ds(x_addr(-ring, strip_cols[k] + tap - 10), 32, stride=pitch), :]
                    lhs[pl.ds(32 * n, 32), pl.ds(tap * 128, 128)] = v.astype(BF16)
                for i in range(0, nr, 2):
                    pieces = []
                    for r in range(r0 + i, min(r0 + i + 2, r0 + nr)):
                        if tap < 9:
                            dr, dc = tap // 3 - 1, tap % 3 - 1
                            pieces.append(hb[pl.ds(h_addr(r + dr, dc), cols), :])
                        else:
                            pieces.append(xg[pl.ds(x_addr(r, tap - 10), cols), :])
                    v = jnp.concatenate(pieces, axis=0) if len(pieces) > 1 else pieces[0]
                    lhs[pl.ds(base + i * cols, len(pieces) * cols), pl.ds(tap * 128, 128)] = v.astype(BF16)

        def matmul(j, ch):
            r0, nr, strips = chunk_list(BLOCK - 1 - j)[ch]
            m = -(-(32 * len(strips) + nr * cols) // 16) * 16
            gss[ch][pl.ds(0, m), :] = jnp.dot(lhss[ch][pl.ds(0, m), :], wall[...], preferred_element_type=F32)

        def cell(g_ref, m0, n, c):
            b = bias_ref[...]
            acts = []
            for q in range(4):
                g = g_ref[pl.ds(m0, n), pl.ds(q * hid, hid)] + b[:, q * hid:(q + 1) * hid]
                acts.append(jnp.tanh(g) if q == 3 else 0.5 * jnp.tanh(0.5 * g) + 0.5)
            c_new = acts[1] * c + acts[0] * acts[3]
            return acts[2] * jnp.tanh(c_new), c_new

        def elementwise(s, j, ch):
            ext = BLOCK - 1 - j
            dst = hbs[s][(j + 1) % BLOCK]
            r0, nr, strips = chunk_list(ext)[ch]
            base = 32 * len(strips)
            for n, k in enumerate(strips):
                h, c_new = cell(gss[ch], 32 * n, 32, css[s][pl.ds(32 * k, 32), :])
                css[s][pl.ds(32 * k, 32), :] = c_new
                h = h * smask[0 if strip_cols[k] < 0 else 1]
                dst[pl.ds(h_addr(-ring, strip_cols[k]), 32, stride=pitch), :] = h.astype(BF16).astype(F32)
            r = r0
            while r < r0 + nr:
                inside = 0 <= r < rows
                cnt = 2 if inside else 1
                crow = (r + ring) * cols
                h, c_new = cell(gss[ch], base + (r - r0) * cols, cnt * cols, cms[s][pl.ds(crow, cnt * cols), :])
                cms[s][pl.ds(crow, cnt * cols), :] = c_new
                if not inside:
                    h = h * (top_ok if r < 0 else bot_ok)
                hb16 = h.astype(BF16)
                if inside:
                    ob[s, j, pl.ds(r * cols, cnt * cols), :] = hb16
                h = hb16.astype(F32)
                for i in range(cnt):
                    dst[pl.ds(h_addr(r + i, 0), cols), :] = h[i * cols:(i + 1) * cols]
                r += cnt

        def out_copy(s, j, b):
            return pltpu.make_async_copy(ob.at[s, j], hout.at[b * BLOCK + j, s], osem.at[s, j])

        def block(b, _):
            par = lax.rem(b, 2)
            for s in range(seqs):
                wait_recv(s, par)
                if s == 0:
                    for j in range(BLOCK):
                        for k in range(8):
                            @pl.when(exists(k))
                            def _():
                                x_copy(b * BLOCK + j, opposite(k)).wait_recv()

                @pl.when(b > 0)
                def _():
                    for j in range(BLOCK):
                        out_copy(s, j, b - 1).wait()

                unpack(s, par)
                late = None
                for j in range(BLOCK):
                    build_xg(s, b * BLOCK + j, BLOCK - 1 - j)
                    for ch in range(3):
                        build_lhs(s, j, ch)
                        matmul(j, ch)
                        if late is not None:
                            elementwise(s, *late)
                        late = (j, ch)
                elementwise(s, *late)
                wait_send(s)

                @pl.when(b < nblock - 1)
                def _():
                    pack(s)
                    send(s, 1 - par)

                for j in range(BLOCK):
                    out_copy(s, j, b).start()
            return 0

        lax.fori_loop(0, nblock, block, 0)

        fin = [pltpu.make_async_copy(cms[s].at[pl.ds(ring * cols, rows * cols), :], cout.at[s], lsem.at[3 + s]) for s in range(seqs)]
        for cp in fin:
            cp.start()
        for t in range(steps):
            for k in range(8):
                @pl.when(exists(k))
                def _():
                    x_copy(t, k).wait_send()
        for s in range(seqs):
            for j in range(BLOCK):
                out_copy(s, j, nblock - 1).wait()
        for cp in fin:
            cp.wait()

    hbuf = pltpu.VMEM((hrows * pitch, hid), F32)
    xbuf = pltpu.VMEM((hrows * pitch, 128), F32)
    mmax = [-(-max(32 * len(chunk_list(e)[ch][2]) + chunk_list(e)[ch][1] * cols for e in range(BLOCK)) // 16) * 16 for ch in range(3)]
    scratch = (
        [hbuf] * 6 + [xbuf] * 2
        + [pltpu.VMEM(((rows + 2 * ring) * cols, hid), F32)] * 2
        + [pltpu.VMEM((nstrip * 32, hid), F32)] * 2
        + [
            pltpu.VMEM((steps * seqs, pitch, (rows + 16) * chan), F32),
            pltpu.VMEM((steps * seqs, rows * chan, cols), BF16),
            pltpu.VMEM((kdim, gates), BF16),
        ]
        + [pltpu.VMEM((mmax[ch], kdim), BF16) for ch in range(3)]
        + [pltpu.VMEM((mmax[ch], gates), F32) for ch in range(3)]
        + [
            pltpu.VMEM((seqs, BLOCK, rows * cols, hid), BF16),
            pltpu.VMEM((seqs, rows * cols, hid), BF16),
            pltpu.VMEM((seqs, 4, 80, hid), BF16),
            pltpu.VMEM((seqs, 4, ring * cols, hid), F32),
            pltpu.VMEM((seqs, 4, 16, hid), BF16),
            pltpu.VMEM((seqs, 4, 8, hid), F32),
            pltpu.VMEM((2, seqs, 4, 80, hid), BF16),
            pltpu.VMEM((2, seqs, 4, ring * cols, hid), F32),
            pltpu.VMEM((2, seqs, 4, 16, hid), BF16),
            pltpu.VMEM((2, seqs, 4, 8, hid), F32),
            pltpu.VMEM((16, hid), F32),
            pltpu.VMEM((2, 32, hid), F32),
            pltpu.SemaphoreType.DMA((5,)),
            pltpu.SemaphoreType.DMA((seqs, BLOCK)),
            pltpu.SemaphoreType.DMA((seqs, 8, 2)),
            pltpu.SemaphoreType.DMA((2, seqs, 8, 2)),
            pltpu.SemaphoreType.DMA((steps, 8)),
            pltpu.SemaphoreType.DMA((steps, 8)),
        ]
    )
    return kernel, scratch


def solution(mesh):
    row_count = mesh.shape["rows"]
    col_count = mesh.shape["cols"]
    frame_spec = P(None, "batch", "rows", "cols", None)
    state_spec = P("batch", "rows", "cols", None)

    def local_run(frames, w_x, w_h, gate_bias, h_init, c_init):
        steps, seqs, rows, cols, chan = frames.shape
        hid = h_init.shape[-1]
        gates = 4 * hid
        kernel, scratch = make_kernel(steps, seqs, rows, cols, chan, hid, row_count, col_count)
        anyspace = pl.BlockSpec(memory_space=pl.ANY)
        vmem = pl.BlockSpec(memory_space=pltpu.VMEM)
        ft = frames.transpose(0, 1, 2, 4, 3).reshape(steps * seqs, rows * chan, cols)
        all_hidden, cell_last = pl.pallas_call(
            kernel,
            out_shape=(
                jax.ShapeDtypeStruct((steps, seqs, rows * cols, hid), BF16),
                jax.ShapeDtypeStruct((seqs, rows * cols, hid), F32),
            ),
            in_specs=[anyspace, vmem, anyspace, vmem, anyspace, anyspace],
            out_specs=(anyspace, anyspace),
            scratch_shapes=scratch,
            compiler_params=pltpu.CompilerParams(collective_id=0, has_side_effects=True, vmem_limit_bytes=60 * 1024 * 1024),
        )(
            ft, w_x, w_h.reshape(9 * hid, gates), gate_bias.reshape(1, gates),
            h_init.reshape(seqs, rows * cols, hid), c_init.reshape(seqs, rows * cols, hid),
        )
        return all_hidden.reshape(steps, seqs, rows, cols, hid), cell_last.reshape(seqs, rows, cols, hid)

    return jax.shard_map(local_run, mesh=mesh, in_specs=(frame_spec, P(), P(), P(), state_spec, state_spec), out_specs=(frame_spec, state_spec), check_vma=False)
```

```python
import jax
import jax.numpy as jnp
from jax import lax
from jax.experimental import pallas as pl
from jax.experimental.pallas import tpu as pltpu
from jax.sharding import PartitionSpec as P

BLOCK = 3
COL0 = 8
DIRS = ((-1, 0), (1, 0), (0, -1), (0, 1), (-1, -1), (-1, 1), (1, -1), (1, 1))
MESH = pl.DeviceIdType.MESH
F32 = jnp.float32
BF16 = jnp.bfloat16


def opposite(k):
    return DIRS.index((-DIRS[k][0], -DIRS[k][1]))


def make_kernel(steps, seqs, rows, cols, chan, hid, row_count, col_count):
    nblock = steps // BLOCK
    pitch = cols + 16
    hrows = rows + 2 * BLOCK + 6
    ring = BLOCK - 1
    xrow0 = 8
    nstrip = 2 * ring
    gates = 4 * hid
    kdim = 9 * hid + 3 * 128
    strip_cols = tuple(range(-ring, 0)) + tuple(range(cols, cols + ring))
    third = rows // 3

    def chunk_list(ext):
        own = [c for c in range(nstrip) if -ext <= strip_cols[c] < cols + ext]
        return (
            (-ext, third + ext, ()),
            (third, third, tuple(own)),
            (2 * third, third + ext, ()),
        )

    def kernel(frames, wx_hbm, wh_hbm, bias_hbm, hinit, cinit, hout, cout, *scratch):
        (hb0a, hb1a, hb2a, hb0b, hb1b, hb2b, xga, xgb, cma, cmb, csa, csb, xt, fbuf, wall,
         lhs0, lhs1, lhs2, gs0, gs1, gs2, wx_ref, bias_ref, hin, sh, sc, sch, scc, rh, rc, rch, rcc, tmp, smask,
         lsem, ssem, rsem, xssem, xrsem) = scratch
        hbs = ((hb0a, hb1a, hb2a), (hb0b, hb1b, hb2b))
        xgs = (xga, xgb)
        cms = (cma, cmb)
        css = (csa, csb)
        lhss = (lhs0, lhs1, lhs2)
        gss = (gs0, gs1, gs2)

        ri = lax.axis_index("rows")
        ci = lax.axis_index("cols")

        def exists(k):
            dr, dc = DIRS[k]
            conds = []
            if dr < 0:
                conds.append(ri > 0)
            if dr > 0:
                conds.append(ri < row_count - 1)
            if dc < 0:
                conds.append(ci > 0)
            if dc > 0:
                conds.append(ci < col_count - 1)
            out = conds[0]
            for extra in conds[1:]:
                out = jnp.logical_and(out, extra)
            return out

        def dev(k):
            return {"rows": ri + DIRS[k][0], "cols": ci + DIRS[k][1]}

        def h_addr(r, c):
            return (r + BLOCK) * pitch + COL0 + c

        def x_addr(r, c):
            return (r + ring) * pitch + COL0 + c

        cp_h = pltpu.make_async_copy(hinit, hin, lsem.at[0])
        near = BLOCK * seqs
        far = steps * seqs - near
        cp_f = pltpu.make_async_copy(frames.at[pl.ds(0, near)], fbuf.at[pl.ds(0, near)], lsem.at[1])
        cp_g = pltpu.make_async_copy(frames.at[pl.ds(near, far)], fbuf.at[pl.ds(near, far)], lsem.at[5])
        cp_w = pltpu.make_async_copy(wh_hbm, wall.at[pl.ds(0, 9 * hid), :], lsem.at[2])
        cp_c = [pltpu.make_async_copy(cinit.at[s], cms[s].at[pl.ds(ring * cols, rows * cols), :], lsem.at[3 + s]) for s in range(seqs)]
        cp_small = [pltpu.make_async_copy(wx_hbm, wx_ref, lsem.at[6]), pltpu.make_async_copy(bias_hbm, bias_ref, lsem.at[7])]
        cp_h.start()
        for s in range(seqs):
            cp_c[s].start()
        cp_f.start()
        cp_w.start()
        for cp in cp_small:
            cp.start()
        cp_g.start()

        barrier = pltpu.get_barrier_semaphore()
        rh[...] = jnp.zeros_like(rh)
        rc[...] = jnp.zeros_like(rc)
        rch[...] = jnp.zeros_like(rch)
        rcc[...] = jnp.zeros_like(rcc)

        xlanes = xt.shape[2]

        def zero_x(i, _):
            for sub in (0, COL0 + cols):
                xt[i, pl.ds(sub, 8), :] = jnp.zeros((8, xlanes), F32)
            for lane0 in (0, xlanes - 128):
                xt[i, pl.ds(COL0, cols), pl.ds(lane0, 128)] = jnp.zeros((cols, 128), F32)
            return 0

        lax.fori_loop(0, steps * seqs, zero_x, 0)
        for k in range(8):
            @pl.when(exists(k))
            def _():
                pl.semaphore_signal(barrier, 1, device_id=dev(k), device_id_type=MESH)
        top_ok = jnp.where(ri > 0, 1.0, 0.0).astype(F32)
        bot_ok = jnp.where(ri < row_count - 1, 1.0, 0.0).astype(F32)
        left_ok = jnp.where(ci > 0, 1.0, 0.0).astype(F32)
        right_ok = jnp.where(ci < col_count - 1, 1.0, 0.0).astype(F32)
        srow = lax.broadcasted_iota(jnp.int32, (32, hid), 0)
        rmask = jnp.where(srow < ring, top_ok, jnp.where(srow >= rows + ring, bot_ok, 1.0))
        smask[0] = rmask * left_ok
        smask[1] = rmask * right_ok

        n_row = jnp.where(ri > 0, 1, 0) + jnp.where(ri < row_count - 1, 1, 0)
        n_col = jnp.where(ci > 0, 1, 0) + jnp.where(ci < col_count - 1, 1, 0)
        pl.semaphore_wait(barrier, (n_row + 1) * (n_col + 1) - 1)

        def msg_copies(s, k, par):
            if k < 4:
                pairs = ((sh.at[s, k], rh.at[par, s, k]), (sc.at[s, k], rc.at[par, s, k]))
            else:
                pairs = ((sch.at[s, k - 4], rch.at[par, s, k - 4]), (scc.at[s, k - 4], rcc.at[par, s, k - 4]))
            return [
                pltpu.make_async_remote_copy(src_ref=a, dst_ref=b, send_sem=ssem.at[s], recv_sem=rsem.at[par, s], device_id=dev(k), device_id_type=MESH)
                for n, (a, b) in enumerate(pairs)
            ]

        def pack(s):
            hb = hbs[s][0]
            cm = cms[s]
            for k in range(8):
                dr, dc = DIRS[k]
                r0 = 0 if dr < 0 else rows - BLOCK
                rc0 = 0 if dr < 0 else rows - ring
                c0 = 0 if dc < 0 else cols - BLOCK
                cc0 = 0 if dc < 0 else cols - ring
                if dc == 0:
                    v = jnp.concatenate([hb[pl.ds(h_addr(r0 + i, 0), cols), :] for i in range(BLOCK)], axis=0)
                    sh[s, k, pl.ds(0, BLOCK * cols), :] = v.astype(BF16)
                    sc[s, k] = cm[pl.ds((rc0 + ring) * cols, ring * cols), :]
                elif dr == 0:
                    v = jnp.concatenate([hb[pl.ds(h_addr(0, c0 + j), rows, stride=pitch), :] for j in range(BLOCK)], axis=0)
                    sh[s, k, pl.ds(0, BLOCK * rows), :] = v.astype(BF16)
                    for j in range(ring):
                        sc[s, k, pl.ds(j * rows, rows), :] = cm[pl.ds(ring * cols + cc0 + j, rows, stride=cols), :]
                else:
                    for i in range(BLOCK):
                        tmp[pl.ds(i * BLOCK, BLOCK), :] = hb[pl.ds(h_addr(r0 + i, c0), BLOCK), :]
                    sch[s, k - 4] = tmp[pl.ds(0, 16), :].astype(BF16)
                    for j in range(ring):
                        scc[s, k - 4, pl.ds(j * ring, ring), :] = cm[pl.ds((rc0 + ring) * cols + cc0 + j, ring, stride=cols), :]

        def unpack(s, par):
            hb = hbs[s][0]
            cm = cms[s]
            cs = css[s]
            for k in range(8):
                dr, dc = DIRS[k]
                o = opposite(k)
                r0 = -BLOCK if dr < 0 else rows
                c0 = -BLOCK if dc < 0 else cols
                st0 = 0 if dc < 0 else ring
                q0 = 0 if dr < 0 else rows + ring
                if dc == 0:
                    v = rh[par, s, o, pl.ds(0, BLOCK * cols), :].astype(F32)
                    for i in range(BLOCK):
                        hb[pl.ds(h_addr(r0 + i, 0), cols), :] = v[i * cols:(i + 1) * cols]
                    cm[pl.ds(q0 * cols, ring * cols), :] = rc[par, s, o]
                elif dr == 0:
                    v = rh[par, s, o, pl.ds(0, BLOCK * rows), :].astype(F32)
                    for j in range(BLOCK):
                        hb[pl.ds(h_addr(0, c0 + j), rows, stride=pitch), :] = v[j * rows:(j + 1) * rows]
                    for j in range(ring):
                        cs[pl.ds((st0 + j) * 32 + ring, rows), :] = rc[par, s, o, pl.ds(j * rows, rows), :]
                else:
                    tmp[pl.ds(0, 16), :] = rch[par, s, o - 4].astype(F32)
                    for i in range(BLOCK):
                        hb[pl.ds(h_addr(r0 + i, c0), BLOCK), :] = tmp[pl.ds(i * BLOCK, BLOCK), :]
                    for j in range(ring):
                        cs[pl.ds((st0 + j) * 32 + q0, ring), :] = rcc[par, s, o - 4, pl.ds(j * ring, ring), :]

        def send(s, par, more=None):
            for k in range(8):
                @pl.when(exists(k) if more is None else jnp.logical_and(exists(k), more))
                def _():
                    for cp in msg_copies(s, k, par):
                        cp.start()

        def wait_all(sem, side, corner, more=None):
            for a in ((1, 2) if row_count > 2 else (row_count - 1,)):
                for b in ((1, 2) if col_count > 2 else (col_count - 1,)):
                    n = side * (a + b) + corner * a * b
                    cond = jnp.logical_and(n_row == a, n_col == b)

                    @pl.when(cond if more is None else jnp.logical_and(cond, more))
                    def _():
                        pltpu.make_async_copy(cinit.at[0, pl.ds(0, n)], cma.at[pl.ds(0, n)], sem).wait()

        msg_side, msg_corner = 40 + ring * cols, 16
        x_side, x_corner = seqs * cols, seqs * 8

        own_lane = xrow0 * chan
        row_lanes = rows * chan

        def x_copy(t, k):
            dr, dc = DIRS[k]
            if dr == 0:
                lanes_s, lanes_d, lane_n = own_lane, own_lane, row_lanes
            else:
                lane_n = 8 * chan
                lanes_s = own_lane if dr < 0 else own_lane + row_lanes - lane_n
                lanes_d = own_lane + row_lanes if dr < 0 else 0
            if dc == 0:
                sub_s, sub_d, sub_n = COL0, COL0, cols
            else:
                sub_n = 8
                sub_s = COL0 if dc < 0 else COL0 + cols - 8
                sub_d = COL0 + cols if dc < 0 else 0
            return pltpu.make_async_remote_copy(
                src_ref=xt.at[pl.ds(t * seqs, seqs), pl.ds(sub_s, sub_n), pl.ds(lanes_s, lane_n)],
                dst_ref=xt.at[pl.ds(t * seqs, seqs), pl.ds(sub_d, sub_n), pl.ds(lanes_d, lane_n)],
                send_sem=xssem.at[lax.rem(t, BLOCK)], recv_sem=xrsem.at[lax.rem(lax.div(t, BLOCK), 2), lax.rem(t, BLOCK)], device_id=dev(k), device_id_type=MESH)

        def load_state(s):
            for r in range(0, rows, 2):
                v = hin[s, pl.ds(r * cols, 2 * cols), :].astype(F32)
                for i in range(2):
                    hbs[s][0][pl.ds(h_addr(r + i, 0), cols), :] = v[i * cols:(i + 1) * cols]

        cp_h.wait()
        load_state(0)
        cp_c[0].wait()
        pack(0)
        send(0, 0)

        eye = (lax.broadcasted_iota(jnp.int32, (cols, cols), 0) == lax.broadcasted_iota(jnp.int32, (cols, cols), 1)).astype(F32).astype(BF16)

        def prep_x(t):
            for s in range(seqs):
                xt[t * seqs + s, pl.ds(COL0, cols), pl.ds(own_lane, row_lanes)] = lax.dot_general(
                    eye, fbuf[t * seqs + s], (((1,), (1,)), ((), ())), preferred_element_type=F32)

        def send_x(t, more=None):
            for k in range(8):
                @pl.when(exists(k) if more is None else jnp.logical_and(exists(k), more))
                def _():
                    x_copy(t, k).start()

        cp_f.wait()
        for t in range(BLOCK):
            prep_x(t)
        for t in range(BLOCK):
            send_x(t)
        load_state(1)
        cp_c[1].wait()
        cp_g.wait()

        cp_w.wait()
        for cp in cp_small:
            cp.wait()
        wall[pl.ds(9 * hid, 3 * 128), :] = jnp.zeros((3 * 128, gates), BF16)
        for dc in range(3):
            for dr in range(3):
                wall[pl.ds(9 * hid + dc * 128 + dr * chan, chan), :] = wx_ref[dr, dc]

        lane = lax.broadcasted_iota(jnp.int32, (pitch, 128), 1)

        def build_xg(s, t, ext):
            xg = xgs[s]
            for r in range(-ext, rows + ext):
                start = r - 1 + xrow0
                g, off = divmod(start, 8)
                v = xt[t * seqs + s, :, pl.ds(g * 128, 128)]
                if off:
                    v = pltpu.roll(v, 128 - chan * off, 1)
                    if off > 5:
                        w = pltpu.roll(xt[t * seqs + s, :, pl.ds((g + 1) * 128, 128)], 128 - chan * off, 1)
                        v = jnp.where(lane < 128 - chan * off, v, w)
                xg[pl.ds(x_addr(r, -COL0), pitch), :] = v

        def build_lhs(s, j, ch):
            hb = hbs[s][j]
            xg = xgs[s]
            r0, nr, strips = chunk_list(BLOCK - 1 - j)[ch]
            lhs = lhss[ch]
            base = 32 * len(strips)
            for tap in range(12):
                for n, k in enumerate(strips):
                    if tap < 9:
                        dr, dc = tap // 3 - 1, tap % 3 - 1
                        v = hb[pl.ds(h_addr(-ring + dr, strip_cols[k] + dc), 32, stride=pitch), :]
                    else:
                        v = xg[pl.ds(x_addr(-ring, strip_cols[k] + tap - 10), 32, stride=pitch), :]
                    lhs[pl.ds(32 * n, 32), pl.ds(tap * 128, 128)] = v.astype(BF16)
                for i in range(0, nr, 2):
                    pieces = []
                    for r in range(r0 + i, min(r0 + i + 2, r0 + nr)):
                        if tap < 9:
                            dr, dc = tap // 3 - 1, tap % 3 - 1
                            pieces.append(hb[pl.ds(h_addr(r + dr, dc), cols), :])
                        else:
                            pieces.append(xg[pl.ds(x_addr(r, tap - 10), cols), :])
                    v = jnp.concatenate(pieces, axis=0) if len(pieces) > 1 else pieces[0]
                    lhs[pl.ds(base + i * cols, len(pieces) * cols), pl.ds(tap * 128, 128)] = v.astype(BF16)

        def matmul(j, ch):
            r0, nr, strips = chunk_list(BLOCK - 1 - j)[ch]
            m = -(-(32 * len(strips) + nr * cols) // 16) * 16
            gss[ch][pl.ds(0, m), :] = jnp.dot(lhss[ch][pl.ds(0, m), :], wall[...], preferred_element_type=F32)

        def cell(g_ref, m0, n, c):
            b = bias_ref[...]
            acts = []
            for q in range(4):
                g = g_ref[pl.ds(m0, n), pl.ds(q * hid, hid)] + b[:, q * hid:(q + 1) * hid]
                acts.append(jnp.tanh(g) if q == 3 else 0.5 * jnp.tanh(0.5 * g) + 0.5)
            c_new = acts[1] * c + acts[0] * acts[3]
            return acts[2] * jnp.tanh(c_new), c_new

        def elementwise(s, j, ch, t, skip=None):
            ext = BLOCK - 1 - j
            dst = hbs[s][(j + 1) % BLOCK]
            r0, nr, strips = chunk_list(ext)[ch]
            base = 32 * len(strips)
            for n, k in enumerate(strips):
                h, c_new = cell(gss[ch], 32 * n, 32, css[s][pl.ds(32 * k, 32), :])
                css[s][pl.ds(32 * k, 32), :] = c_new
                h = h * smask[0 if strip_cols[k] < 0 else 1]
                dst[pl.ds(h_addr(-ring, strip_cols[k]), 32, stride=pitch), :] = h.astype(BF16).astype(F32)
            r = r0
            while r < r0 + nr:
                inside = 0 <= r < rows
                cnt = 2 if inside else 1
                crow = (r + ring) * cols
                c_old = cms[s][pl.ds(crow, cnt * cols), :]
                h, c_new = cell(gss[ch], base + (r - r0) * cols, cnt * cols, c_old)
                if skip is not None:
                    c_new = jnp.where(skip, c_old, c_new)
                cms[s][pl.ds(crow, cnt * cols), :] = c_new
                if not inside:
                    h = h * (top_ok if r < 0 else bot_ok)
                hb16 = h.astype(BF16)
                if inside:
                    hout[t, s, pl.ds(r * cols, cnt * cols), :] = hb16
                h = hb16.astype(F32)
                for i in range(cnt):
                    new = h[i * cols:(i + 1) * cols]
                    if skip is not None:
                        new = jnp.where(skip, dst[pl.ds(h_addr(r + i, 0), cols), :], new)
                    dst[pl.ds(h_addr(r + i, 0), cols), :] = new
                r += cnt

        last = (BLOCK - 1, 2)

        def block(b, _):
            par = lax.rem(b, 2)
            for s in range(seqs):
                o = 1 - s
                wait_all(rsem.at[par, s], msg_side, msg_corner)
                if s == 0:
                    for j in range(BLOCK):
                        wait_all(xrsem.at[par, j], x_side, x_corner)
                        wait_all(xssem.at[j], x_side, x_corner)
                    wait_all(ssem.at[o], msg_side, msg_corner, b > 0)
                else:
                    wait_all(ssem.at[o], msg_side, msg_corner)
                unpack(s, par)
                build_xg(s, b * BLOCK, BLOCK - 1)
                build_lhs(s, 0, 0)
                if s == 0:
                    elementwise(o, *last, lax.rem(b * BLOCK - 1 + steps, steps), b == 0)
                    pack(o)
                    send(o, par)
                else:
                    elementwise(o, *last, b * BLOCK + BLOCK - 1)
                    pack(o)
                    send(o, 1 - par, b < nblock - 1)
                late = None
                for j in range(BLOCK):
                    if j > 0:
                        build_xg(s, b * BLOCK + j, BLOCK - 1 - j)
                    if s == 0 and j == BLOCK - 1:
                        for q in range(BLOCK):
                            prep_x(lax.rem((b + 1) * BLOCK + q, steps))
                        for q in range(BLOCK):
                            send_x(lax.rem((b + 1) * BLOCK + q, steps), b < nblock - 1)
                    for ch in range(3):
                        if j + ch > 0:
                            build_lhs(s, j, ch)
                        matmul(j, ch)
                        if late is not None:
                            elementwise(s, *late, b * BLOCK + late[0])
                        late = (j, ch)
            return 0

        lax.fori_loop(0, nblock, block, 0)
        elementwise(1, *last, steps - 1)
        wait_all(ssem.at[1], msg_side, msg_corner)
        for s in range(seqs):
            cout[s] = cms[s][pl.ds(ring * cols, rows * cols), :]

    hbuf = pltpu.VMEM((hrows * pitch, hid), F32)
    xbuf = pltpu.VMEM((hrows * pitch, 128), F32)
    mmax = [-(-max(32 * len(chunk_list(e)[ch][2]) + chunk_list(e)[ch][1] * cols for e in range(BLOCK)) // 16) * 16 for ch in range(3)]
    scratch = (
        [hbuf] * 6 + [xbuf] * 2
        + [pltpu.VMEM(((rows + 2 * ring) * cols, hid), F32)] * 2
        + [pltpu.VMEM((nstrip * 32, hid), F32)] * 2
        + [
            pltpu.VMEM((steps * seqs, pitch, (rows + 16) * chan), F32),
            pltpu.VMEM((steps * seqs, rows * chan, cols), BF16),
            pltpu.VMEM((kdim, gates), BF16),
        ]
        + [pltpu.VMEM((mmax[ch], kdim), BF16) for ch in range(3)]
        + [pltpu.VMEM((mmax[ch], gates), F32) for ch in range(3)]
        + [
            pltpu.VMEM((3, 3, chan, gates), BF16),
            pltpu.VMEM((1, gates), F32),
            pltpu.VMEM((seqs, rows * cols, hid), BF16),
            pltpu.VMEM((seqs, 4, 80, hid), BF16),
            pltpu.VMEM((seqs, 4, ring * cols, hid), F32),
            pltpu.VMEM((seqs, 4, 16, hid), BF16),
            pltpu.VMEM((seqs, 4, 8, hid), F32),
            pltpu.VMEM((2, seqs, 4, 80, hid), BF16),
            pltpu.VMEM((2, seqs, 4, ring * cols, hid), F32),
            pltpu.VMEM((2, seqs, 4, 16, hid), BF16),
            pltpu.VMEM((2, seqs, 4, 8, hid), F32),
            pltpu.VMEM((16, hid), F32),
            pltpu.VMEM((2, 32, hid), F32),
            pltpu.SemaphoreType.DMA((8,)),
            pltpu.SemaphoreType.DMA((seqs,)),
            pltpu.SemaphoreType.DMA((2, seqs)),
            pltpu.SemaphoreType.DMA((BLOCK,)),
            pltpu.SemaphoreType.DMA((2, BLOCK)),
        ]
    )
    return kernel, scratch


def solution(mesh):
    row_count = mesh.shape["rows"]
    col_count = mesh.shape["cols"]
    frame_spec = P(None, "batch", "rows", "cols", None)
    state_spec = P("batch", "rows", "cols", None)

    def local_run(frames, w_x, w_h, gate_bias, h_init, c_init):
        steps, seqs, rows, cols, chan = frames.shape
        hid = h_init.shape[-1]
        gates = 4 * hid
        kernel, scratch = make_kernel(steps, seqs, rows, cols, chan, hid, row_count, col_count)
        hbm = pl.BlockSpec(memory_space=pltpu.HBM)
        vmem = pl.BlockSpec(memory_space=pltpu.VMEM)
        ft = frames.transpose(0, 1, 2, 4, 3).reshape(steps * seqs, rows * chan, cols)
        all_hidden, cell_last = pl.pallas_call(
            kernel,
            out_shape=(
                pltpu.VMEM((steps, seqs, rows * cols, hid), BF16),
                pltpu.VMEM((seqs, rows * cols, hid), F32),
            ),
            in_specs=[hbm] * 6,
            out_specs=(vmem, vmem),
            scratch_shapes=scratch,
            compiler_params=pltpu.CompilerParams(collective_id=0, has_side_effects=True, vmem_limit_bytes=44 * 1024 * 1024),
        )(
            *[
                pltpu.with_memory_space_constraint(x, pltpu.HBM)
                for x in (
                    ft, w_x, w_h.reshape(9 * hid, gates), gate_bias.reshape(1, gates),
                    h_init.reshape(seqs, rows * cols, hid), c_init.reshape(seqs, rows * cols, hid),
                )
            ]
        )
        return all_hidden.reshape(steps, seqs, rows, cols, hid), cell_last.reshape(seqs, rows, cols, hid)

    return jax.shard_map(local_run, mesh=mesh, in_specs=(frame_spec, P(), P(), P(), state_spec, state_spec), out_specs=(frame_spec, state_spec), check_vma=False)
```

```python
import jax
import jax.numpy as jnp
from jax import lax
from jax.experimental import pallas as pl
from jax.experimental.pallas import tpu as pltpu
from jax.sharding import PartitionSpec as P

BLOCK = 3
COL0 = 8
DIRS = ((-1, 0), (1, 0), (0, -1), (0, 1), (-1, -1), (-1, 1), (1, -1), (1, 1))
MESH = pl.DeviceIdType.MESH
F32 = jnp.float32
BF16 = jnp.bfloat16


def opposite(k):
    return DIRS.index((-DIRS[k][0], -DIRS[k][1]))


def make_kernel(steps, seqs, rows, cols, chan, hid, row_count, col_count):
    nblock = steps // BLOCK
    pitch = cols + 16
    hrows = rows + 2 * BLOCK + 6
    ring = BLOCK - 1
    xrow0 = 8
    nstrip = 2 * ring
    gates = 4 * hid
    kdim = 9 * hid + 3 * 128
    strip_cols = tuple(range(-ring, 0)) + tuple(range(cols, cols + ring))
    third = rows // 3

    def chunk_list(ext):
        own = [c for c in range(nstrip) if -ext <= strip_cols[c] < cols + ext]
        return (
            (-ext, third + ext, ()),
            (third, third, tuple(own)),
            (2 * third, third + ext, ()),
        )

    def kernel(frames, wx_hbm, wh_hbm, bias_hbm, hinit, cinit, hout, cout, *scratch):
        (hb0a, hb1a, hb2a, hb0b, hb1b, hb2b, xga, xgb, cma, cmb, csa, csb, xt, fbuf, wall,
         lhs0, lhs1, lhs2, gs0, gs1, gs2, wx_ref, bias_ref, hin, sh, sc, sq, rh, rc, rq, smask,
         lsem, ssem, rsem, xssem, xrsem) = scratch
        hbs = ((hb0a, hb1a, hb2a), (hb0b, hb1b, hb2b))
        xgs = (xga, xgb)
        cms = (cma, cmb)
        css = (csa, csb)
        lhss = (lhs0, lhs1, lhs2)
        gss = (gs0, gs1, gs2)

        ri = lax.axis_index("rows")
        ci = lax.axis_index("cols")

        def exists(k):
            dr, dc = DIRS[k]
            conds = []
            if dr < 0:
                conds.append(ri > 0)
            if dr > 0:
                conds.append(ri < row_count - 1)
            if dc < 0:
                conds.append(ci > 0)
            if dc > 0:
                conds.append(ci < col_count - 1)
            out = conds[0]
            for extra in conds[1:]:
                out = jnp.logical_and(out, extra)
            return out

        def dev(k):
            return {
                "rows": lax.rem(ri + DIRS[k][0] + row_count, row_count),
                "cols": lax.rem(ci + DIRS[k][1] + col_count, col_count),
            }

        present = [exists(k) for k in range(8)]
        n_row = jnp.where(ri > 0, 1, 0) + jnp.where(ri < row_count - 1, 1, 0)
        n_col = jnp.where(ci > 0, 1, 0) + jnp.where(ci < col_count - 1, 1, 0)

        def pick(k, dst, real, spare):
            return jnp.where(jnp.logical_and(present[k], dst < nblock), real, spare)

        def h_addr(r, c):
            return (r + BLOCK) * pitch + COL0 + c

        def x_addr(r, c):
            return (r + ring) * pitch + COL0 + c

        cp_h = pltpu.make_async_copy(hinit, hin, lsem.at[0])
        near = BLOCK * seqs
        far = steps * seqs - near
        cp_f = pltpu.make_async_copy(frames.at[pl.ds(0, near)], fbuf.at[pl.ds(0, near)], lsem.at[1])
        cp_g = pltpu.make_async_copy(frames.at[pl.ds(near, far)], fbuf.at[pl.ds(near, far)], lsem.at[5])
        cp_w = pltpu.make_async_copy(wh_hbm, wall.at[pl.ds(0, 9 * hid), :], lsem.at[2])
        cp_c = [pltpu.make_async_copy(cinit.at[s], cms[s].at[pl.ds(ring * cols, rows * cols), :], lsem.at[3 + s]) for s in range(seqs)]
        cp_small = [pltpu.make_async_copy(wx_hbm, wx_ref, lsem.at[6]), pltpu.make_async_copy(bias_hbm, bias_ref, lsem.at[7])]
        cp_h.start()
        for s in range(seqs):
            cp_c[s].start()
        cp_f.start()
        cp_w.start()
        for cp in cp_small:
            cp.start()
        cp_g.start()

        barrier = pltpu.get_barrier_semaphore()
        for ref in (rh, rc, rq):
            ref[pl.ds(0, 2)] = jnp.zeros((2,) + ref.shape[1:], ref.dtype)

        xlanes = xt.shape[2]

        def zero_x(i, _):
            for sub in (0, COL0 + cols):
                xt[i, pl.ds(sub, 8), :] = jnp.zeros((8, xlanes), F32)
            for lane0 in (0, xlanes - 128):
                xt[i, pl.ds(COL0, cols), pl.ds(lane0, 128)] = jnp.zeros((cols, 128), F32)
            return 0

        lax.fori_loop(0, steps * seqs, zero_x, 0)
        for k in range(8):
            pl.semaphore_signal(barrier, 1, device_id=dev(k), device_id_type=MESH)
        top_ok = jnp.where(ri > 0, 1.0, 0.0).astype(F32)
        bot_ok = jnp.where(ri < row_count - 1, 1.0, 0.0).astype(F32)
        left_ok = jnp.where(ci > 0, 1.0, 0.0).astype(F32)
        right_ok = jnp.where(ci < col_count - 1, 1.0, 0.0).astype(F32)
        srow = lax.broadcasted_iota(jnp.int32, (32, hid), 0)
        rmask = jnp.where(srow < ring, top_ok, jnp.where(srow >= rows + ring, bot_ok, 1.0))
        smask[0] = rmask * left_ok
        smask[1] = rmask * right_ok

        pl.semaphore_wait(barrier, 8)

        def msg_copies(s, k, dst):
            slot = pick(k, dst, lax.rem(dst, 2), 2 + dst)
            sem = pick(k, dst, lax.rem(dst, 2) * seqs + s, 2 * seqs + dst * seqs + s)
            if k < 4:
                pairs = ((sh.at[s, k], rh.at[slot, s, k]), (sc.at[s, k], rc.at[slot, s, k]))
            else:
                pairs = ((sq.at[s, k - 4], rq.at[slot, s, k - 4]),)
            return [
                pltpu.make_async_remote_copy(src_ref=a, dst_ref=b, send_sem=ssem.at[s], recv_sem=rsem.at[sem], device_id=dev(k), device_id_type=MESH)
                for a, b in pairs
            ]

        def pack(s):
            hb = hbs[s][0]
            cm = cms[s]
            for k in range(8):
                dr, dc = DIRS[k]
                r0 = 0 if dr < 0 else rows - BLOCK
                rc0 = 0 if dr < 0 else rows - ring
                c0 = 0 if dc < 0 else cols - BLOCK
                cc0 = 0 if dc < 0 else cols - ring
                if dc == 0:
                    v = jnp.concatenate([hb[pl.ds(h_addr(r0 + i, 0), cols), :] for i in range(BLOCK)], axis=0)
                    sh[s, k, pl.ds(0, BLOCK * cols), :] = v.astype(BF16)
                    sc[s, k] = cm[pl.ds((rc0 + ring) * cols, ring * cols), :]
                elif dr == 0:
                    v = jnp.concatenate([hb[pl.ds(h_addr(0, c0 + j), rows, stride=pitch), :] for j in range(BLOCK)], axis=0)
                    sh[s, k, pl.ds(0, BLOCK * rows), :] = v.astype(BF16)
                    for j in range(ring):
                        sc[s, k, pl.ds(j * rows, rows), :] = cm[pl.ds(ring * cols + cc0 + j, rows, stride=cols), :]
                else:
                    for i in range(BLOCK):
                        sq[s, k - 4, pl.ds(i * BLOCK, BLOCK), :] = hb[pl.ds(h_addr(r0 + i, c0), BLOCK), :]
                    for j in range(ring):
                        sq[s, k - 4, pl.ds(BLOCK * BLOCK + j * ring, ring), :] = cm[pl.ds((rc0 + ring) * cols + cc0 + j, ring, stride=cols), :]

        def unpack(s, par):
            hb = hbs[s][0]
            cm = cms[s]
            cs = css[s]
            for k in range(8):
                dr, dc = DIRS[k]
                o = opposite(k)
                r0 = -BLOCK if dr < 0 else rows
                c0 = -BLOCK if dc < 0 else cols
                st0 = 0 if dc < 0 else ring
                q0 = 0 if dr < 0 else rows + ring
                if dc == 0:
                    v = rh[par, s, o, pl.ds(0, BLOCK * cols), :].astype(F32)
                    for i in range(BLOCK):
                        hb[pl.ds(h_addr(r0 + i, 0), cols), :] = v[i * cols:(i + 1) * cols]
                    cm[pl.ds(q0 * cols, ring * cols), :] = rc[par, s, o]
                elif dr == 0:
                    v = rh[par, s, o, pl.ds(0, BLOCK * rows), :].astype(F32)
                    for j in range(BLOCK):
                        hb[pl.ds(h_addr(0, c0 + j), rows, stride=pitch), :] = v[j * rows:(j + 1) * rows]
                    for j in range(ring):
                        cs[pl.ds((st0 + j) * 32 + ring, rows), :] = rc[par, s, o, pl.ds(j * rows, rows), :]
                else:
                    for i in range(BLOCK):
                        hb[pl.ds(h_addr(r0 + i, c0), BLOCK), :] = rq[par, s, o - 4, pl.ds(i * BLOCK, BLOCK), :]
                    for j in range(ring):
                        cs[pl.ds((st0 + j) * 32 + q0, ring), :] = rq[par, s, o - 4, pl.ds(BLOCK * BLOCK + j * ring, ring), :]

        def send(s, dst):
            for k in range(8):
                for cp in msg_copies(s, k, dst):
                    cp.start()

        def wait_rows(sem, n):
            pltpu.make_async_copy(cinit.at[:, pl.ds(0, n // seqs)], cout.at[:, pl.ds(0, n // seqs)], sem).wait()

        def wait_all(sem, side, corner, absent=False):
            for a in ((1, 2) if row_count > 2 else (row_count - 1,)):
                for b in ((1, 2) if col_count > 2 else (col_count - 1,)):
                    n = side * (a + b) + corner * a * b
                    if absent:
                        n = 4 * side + 4 * corner - n
                    if n:
                        @pl.when(jnp.logical_and(n_row == a, n_col == b))
                        def _():
                            wait_rows(sem, n)

        msg_side, msg_corner = 40 + ring * cols, 16
        x_side, x_corner = BLOCK * seqs * cols, BLOCK * seqs * 8
        msg_total = 4 * (msg_side + msg_corner)
        x_total = 4 * (x_side + x_corner)

        own_lane = xrow0 * chan
        row_lanes = rows * chan

        def x_copy(dst, k):
            dr, dc = DIRS[k]
            if dr == 0:
                lanes_s, lanes_d, lane_n = own_lane, own_lane, row_lanes
            else:
                lane_n = 8 * chan
                lanes_s = own_lane if dr < 0 else own_lane + row_lanes - lane_n
                lanes_d = own_lane + row_lanes if dr < 0 else 0
            if dc == 0:
                sub_s, sub_d, sub_n = COL0, COL0, cols
            else:
                sub_n = 8
                sub_s = COL0 if dc < 0 else COL0 + cols - 8
                sub_d = COL0 + cols if dc < 0 else 0
            return make_x_copy(dst, k, sub_s, sub_d, sub_n, lanes_s, lanes_d, lane_n, xssem.at[0], 0, 0)

        def make_x_copy(dst, k, sub_s, sub_d, sub_n, lanes_s, lanes_d, lane_n, ssem_x, real, spare):
            per = BLOCK * seqs
            return pltpu.make_async_remote_copy(
                src_ref=xt.at[pl.ds(lax.rem(dst, nblock) * per, per), pl.ds(sub_s, sub_n), pl.ds(lanes_s, lane_n)],
                dst_ref=xt.at[pl.ds(pick(k, dst, dst, nblock + dst) * per, per), pl.ds(sub_d, sub_n), pl.ds(lanes_d, lane_n)],
                send_sem=ssem_x, recv_sem=xrsem.at[pick(k, dst, real, XSPARE + spare)], device_id=dev(k), device_id_type=MESH)

        XSPARE = 5

        def x_rows(dst, k):
            up = k == 0
            return make_x_copy(
                dst, k, COL0, COL0, cols, own_lane if up else own_lane + row_lanes - 128, own_lane + row_lanes if up else 0, 128,
                xssem.at[1], 1 + lax.rem(dst, 2), 1 + dst)

        def x_cols(dst, k):
            left = k == 2
            return make_x_copy(
                dst, k, COL0 if left else COL0 + cols - 8, COL0 + cols if left else 0, 8, 0, 0, xlanes,
                xssem.at[2], 3 + lax.rem(dst, 2), 2 + nblock + dst)

        def wait_axis(sem, count, size, more=None, absent=False):
            for a in (0, 1, 2):
                n = (2 - a if absent else a) * size
                cond = count == a
                if n:
                    @pl.when(cond if more is None else jnp.logical_and(cond, more))
                    def _():
                        wait_rows(sem, n)

        xr_size = BLOCK * seqs * cols
        xc_size = BLOCK * seqs * 8 * (xlanes // 128)

        def load_state(s):
            for r in range(0, rows, 2):
                v = hin[s, pl.ds(r * cols, 2 * cols), :].astype(F32)
                for i in range(2):
                    hbs[s][0][pl.ds(h_addr(r + i, 0), cols), :] = v[i * cols:(i + 1) * cols]

        cp_h.wait()
        load_state(0)
        cp_c[0].wait()
        pack(0)
        send(0, 0)

        eye = (lax.broadcasted_iota(jnp.int32, (cols, cols), 0) == lax.broadcasted_iota(jnp.int32, (cols, cols), 1)).astype(F32).astype(BF16)

        def prep_x(dst):
            for q in range(BLOCK):
                t = dst * BLOCK + q
                for s in range(seqs):
                    xt[t * seqs + s, pl.ds(COL0, cols), pl.ds(own_lane, row_lanes)] = lax.dot_general(
                        eye, fbuf[lax.rem(t, steps) * seqs + s], (((1,), (1,)), ((), ())), preferred_element_type=F32)


        cp_f.wait()
        prep_x(0)
        for k in range(8):
            x_copy(0, k).start()
        load_state(1)
        cp_c[1].wait()
        cp_w.wait()
        for cp in cp_small:
            cp.wait()
        wall[pl.ds(9 * hid, 3 * 128), :] = jnp.zeros((3 * 128, gates), BF16)
        for dc in range(3):
            for dr in range(3):
                wall[pl.ds(9 * hid + dc * 128 + dr * chan, chan), :] = wx_ref[dr, dc]

        cp_g.wait()

        def prep_more(dst, _):
            prep_x(dst)
            return 0

        lax.fori_loop(1, nblock, prep_more, 0)
        wait_all(xrsem.at[0], x_side, x_corner)
        lane = lax.broadcasted_iota(jnp.int32, (pitch, 128), 1)

        def build_xg(s, t, ext):
            xg = xgs[s]
            for r in range(-ext, rows + ext):
                start = r - 1 + xrow0
                g, off = divmod(start, 8)
                v = xt[t * seqs + s, :, pl.ds(g * 128, 128)]
                if off:
                    v = pltpu.roll(v, 128 - chan * off, 1)
                    if off > 5:
                        w = pltpu.roll(xt[t * seqs + s, :, pl.ds((g + 1) * 128, 128)], 128 - chan * off, 1)
                        v = jnp.where(lane < 128 - chan * off, v, w)
                xg[pl.ds(x_addr(r, -COL0), pitch), :] = v

        def build_lhs(s, j, ch):
            hb = hbs[s][j]
            xg = xgs[s]
            r0, nr, strips = chunk_list(BLOCK - 1 - j)[ch]
            lhs = lhss[ch]
            base = 32 * len(strips)
            for tap in range(12):
                for n, k in enumerate(strips):
                    if tap < 9:
                        dr, dc = tap // 3 - 1, tap % 3 - 1
                        v = hb[pl.ds(h_addr(-ring + dr, strip_cols[k] + dc), 32, stride=pitch), :]
                    else:
                        v = xg[pl.ds(x_addr(-ring, strip_cols[k] + tap - 10), 32, stride=pitch), :]
                    lhs[pl.ds(32 * n, 32), pl.ds(tap * 128, 128)] = v.astype(BF16)
                for i in range(0, nr, 2):
                    pieces = []
                    for r in range(r0 + i, min(r0 + i + 2, r0 + nr)):
                        if tap < 9:
                            dr, dc = tap // 3 - 1, tap % 3 - 1
                            pieces.append(hb[pl.ds(h_addr(r + dr, dc), cols), :])
                        else:
                            pieces.append(xg[pl.ds(x_addr(r, tap - 10), cols), :])
                    v = jnp.concatenate(pieces, axis=0) if len(pieces) > 1 else pieces[0]
                    lhs[pl.ds(base + i * cols, len(pieces) * cols), pl.ds(tap * 128, 128)] = v.astype(BF16)

        def matmul(j, ch):
            r0, nr, strips = chunk_list(BLOCK - 1 - j)[ch]
            m = -(-(32 * len(strips) + nr * cols) // 16) * 16
            gss[ch][pl.ds(0, m), :] = jnp.dot(lhss[ch][pl.ds(0, m), :], wall[...], preferred_element_type=F32)

        def cell(g_ref, m0, n, c):
            b = bias_ref[...]
            acts = []
            for q in range(4):
                g = g_ref[pl.ds(m0, n), pl.ds(q * hid, hid)] + b[:, q * hid:(q + 1) * hid]
                acts.append(jnp.tanh(g) if q == 3 else 0.5 * jnp.tanh(0.5 * g) + 0.5)
            c_new = acts[1] * c + acts[0] * acts[3]
            return acts[2] * jnp.tanh(c_new), c_new

        def elementwise(s, j, ch, t, skip=None):
            ext = BLOCK - 1 - j
            dst = hbs[s][(j + 1) % BLOCK]
            r0, nr, strips = chunk_list(ext)[ch]
            base = 32 * len(strips)
            for n, k in enumerate(strips):
                h, c_new = cell(gss[ch], 32 * n, 32, css[s][pl.ds(32 * k, 32), :])
                css[s][pl.ds(32 * k, 32), :] = c_new
                h = h * smask[0 if strip_cols[k] < 0 else 1]
                dst[pl.ds(h_addr(-ring, strip_cols[k]), 32, stride=pitch), :] = h.astype(BF16).astype(F32)
            r = r0
            while r < r0 + nr:
                inside = 0 <= r < rows
                cnt = 2 if inside else 1
                crow = (r + ring) * cols
                c_old = cms[s][pl.ds(crow, cnt * cols), :]
                h, c_new = cell(gss[ch], base + (r - r0) * cols, cnt * cols, c_old)
                if skip is not None:
                    c_new = jnp.where(skip, c_old, c_new)
                cms[s][pl.ds(crow, cnt * cols), :] = c_new
                if not inside:
                    h = h * (top_ok if r < 0 else bot_ok)
                hb16 = h.astype(BF16)
                if inside:
                    hout[t, s, pl.ds(r * cols, cnt * cols), :] = hb16
                h = hb16.astype(F32)
                for i in range(cnt):
                    new = h[i * cols:(i + 1) * cols]
                    if skip is not None:
                        new = jnp.where(skip, dst[pl.ds(h_addr(r + i, 0), cols), :], new)
                    dst[pl.ds(h_addr(r + i, 0), cols), :] = new
                r += cnt

        last = (BLOCK - 1, 2)

        def block(b, _):
            par = lax.rem(b, 2)
            for s in range(seqs):
                o = 1 - s
                wait_all(rsem.at[par * seqs + s], msg_side, msg_corner)
                if s == 0:
                    @pl.when(b > 0)
                    def _():
                        wait_rows(ssem.at[o], msg_total)
                        wait_rows(xssem.at[2], 2 * xc_size)

                    wait_axis(xrsem.at[3 + par], n_col, xc_size, b > 0)
                else:
                    wait_rows(ssem.at[o], msg_total)
                    wait_rows(xssem.at[1], 2 * xr_size)
                    wait_axis(xrsem.at[1 + lax.rem(b + 1, 2)], n_row, xr_size, b < nblock - 1)
                unpack(s, par)
                build_xg(s, b * BLOCK, BLOCK - 1)
                build_lhs(s, 0, 0)
                if s == 0:
                    elementwise(o, *last, lax.rem(b * BLOCK - 1 + steps, steps), b == 0)
                    pack(o)
                    send(o, b)
                    for k in (0, 1):
                        x_rows(b + 1, k).start()
                else:
                    elementwise(o, *last, b * BLOCK + BLOCK - 1)
                    pack(o)
                    send(o, b + 1)
                    for k in (2, 3):
                        x_cols(b + 1, k).start()
                late = None
                for j in range(BLOCK):
                    if j > 0:
                        build_xg(s, b * BLOCK + j, BLOCK - 1 - j)
                    for ch in range(3):
                        if j + ch > 0:
                            build_lhs(s, j, ch)
                        matmul(j, ch)
                        if late is not None:
                            elementwise(s, *late, b * BLOCK + late[0])
                        late = (j, ch)
            return 0

        lax.fori_loop(0, nblock, block, 0)
        elementwise(1, *last, steps - 1)
        wait_rows(ssem.at[0], msg_total)
        wait_rows(ssem.at[1], msg_total)
        wait_rows(xssem.at[0], x_total)
        wait_rows(xssem.at[2], 2 * xc_size)
        for dst in range(nblock):
            for s in range(seqs):
                wait_all(rsem.at[(2 + dst) * seqs + s], msg_side, msg_corner, absent=True)
        wait_all(xrsem.at[XSPARE], x_side, x_corner, absent=True)
        for dst in range(1, nblock):
            wait_axis(xrsem.at[XSPARE + 1 + dst], n_row, xr_size, absent=True)
            wait_axis(xrsem.at[XSPARE + 2 + nblock + dst], n_col, xc_size, absent=True)
        wait_rows(rsem.at[(2 + nblock) * seqs], msg_total)
        wait_rows(xrsem.at[XSPARE + 1 + nblock], 2 * xr_size)
        wait_rows(xrsem.at[XSPARE + 2 + 2 * nblock], 2 * xc_size)
        for s in range(seqs):
            cout[s] = cms[s][pl.ds(ring * cols, rows * cols), :]

    hbuf = pltpu.VMEM((hrows * pitch, hid), F32)
    xbuf = pltpu.VMEM((hrows * pitch, 128), F32)
    mmax = [-(-max(32 * len(chunk_list(e)[ch][2]) + chunk_list(e)[ch][1] * cols for e in range(BLOCK)) // 16) * 16 for ch in range(3)]
    scratch = (
        [hbuf] * 6 + [xbuf] * 2
        + [pltpu.VMEM(((rows + 2 * ring) * cols, hid), F32)] * 2
        + [pltpu.VMEM((nstrip * 32, hid), F32)] * 2
        + [
            pltpu.VMEM(((2 * nblock + 1) * BLOCK * seqs, pitch, (rows + 16) * chan), F32),
            pltpu.VMEM((steps * seqs, rows * chan, cols), BF16),
            pltpu.VMEM((kdim, gates), BF16),
        ]
        + [pltpu.VMEM((mmax[ch], kdim), BF16) for ch in range(3)]
        + [pltpu.VMEM((mmax[ch], gates), F32) for ch in range(3)]
        + [
            pltpu.VMEM((3, 3, chan, gates), BF16),
            pltpu.VMEM((1, gates), F32),
            pltpu.VMEM((seqs, rows * cols, hid), BF16),
            pltpu.VMEM((seqs, 4, 80, hid), BF16),
            pltpu.VMEM((seqs, 4, ring * cols, hid), F32),
            pltpu.VMEM((seqs, 4, 16, hid), F32),
            pltpu.VMEM((3 + nblock, seqs, 4, 80, hid), BF16),
            pltpu.VMEM((3 + nblock, seqs, 4, ring * cols, hid), F32),
            pltpu.VMEM((3 + nblock, seqs, 4, 16, hid), F32),
            pltpu.VMEM((2, 32, hid), F32),
            pltpu.SemaphoreType.DMA((8,)),
            pltpu.SemaphoreType.DMA((seqs,)),
            pltpu.SemaphoreType.DMA(((3 + nblock) * seqs,)),
            pltpu.SemaphoreType.DMA((3,)),
            pltpu.SemaphoreType.DMA((8 + 2 * nblock,)),
        ]
    )
    return kernel, scratch


def solution(mesh):
    row_count = mesh.shape["rows"]
    col_count = mesh.shape["cols"]
    frame_spec = P(None, "batch", "rows", "cols", None)
    state_spec = P("batch", "rows", "cols", None)

    def local_run(frames, w_x, w_h, gate_bias, h_init, c_init):
        steps, seqs, rows, cols, chan = frames.shape
        hid = h_init.shape[-1]
        gates = 4 * hid
        kernel, scratch = make_kernel(steps, seqs, rows, cols, chan, hid, row_count, col_count)
        hbm = pl.BlockSpec(memory_space=pltpu.HBM)
        vmem = pl.BlockSpec(memory_space=pltpu.VMEM)
        ft = frames.transpose(0, 1, 2, 4, 3).reshape(steps * seqs, rows * chan, cols)
        all_hidden, cell_last = pl.pallas_call(
            kernel,
            out_shape=(
                pltpu.VMEM((steps, seqs, rows * cols, hid), BF16),
                pltpu.VMEM((seqs, rows * cols, hid), F32),
            ),
            in_specs=[hbm] * 6,
            out_specs=(vmem, vmem),
            scratch_shapes=scratch,
            compiler_params=pltpu.CompilerParams(collective_id=0, has_side_effects=True, vmem_limit_bytes=44 * 1024 * 1024),
        )(
            *[
                pltpu.with_memory_space_constraint(x, pltpu.HBM)
                for x in (
                    ft, w_x, w_h.reshape(9 * hid, gates), gate_bias.reshape(1, gates),
                    h_init.reshape(seqs, rows * cols, hid), c_init.reshape(seqs, rows * cols, hid),
                )
            ]
        )
        return all_hidden.reshape(steps, seqs, rows, cols, hid), cell_last.reshape(seqs, rows, cols, hid)

    return jax.shard_map(local_run, mesh=mesh, in_specs=(frame_spec, P(), P(), P(), state_spec, state_spec), out_specs=(frame_spec, state_spec), check_vma=False)
```

```python
import jax
import jax.numpy as jnp
from jax import lax
from jax.experimental import pallas as pl
from jax.experimental.pallas import tpu as pltpu
from jax.sharding import PartitionSpec as P

BLOCK = 3
COL0 = 8
DIRS = ((-1, 0), (1, 0), (0, -1), (0, 1), (-1, -1), (-1, 1), (1, -1), (1, 1))
MESH = pl.DeviceIdType.MESH
F32 = jnp.float32
BF16 = jnp.bfloat16


def opposite(k):
    return DIRS.index((-DIRS[k][0], -DIRS[k][1]))


def make_kernel(steps, seqs, rows, cols, chan, hid, row_count, col_count):
    nblock = steps // BLOCK
    pitch = cols + 16
    hrows = rows + 2 * BLOCK + 6
    ring = BLOCK - 1
    xrow0 = 8
    nstrip = 2 * ring
    gates = 4 * hid
    kdim = 9 * hid + 3 * 128
    strip_cols = tuple(range(-ring, 0)) + tuple(range(cols, cols + ring))
    third = rows // 3

    def chunk_list(ext):
        own = [c for c in range(nstrip) if -ext <= strip_cols[c] < cols + ext]
        return (
            (-ext, third + ext, ()),
            (third, third, tuple(own)),
            (2 * third, third + ext, ()),
        )

    def kernel(frames, wx_hbm, wh_hbm, bias_hbm, hinit, cinit, hout, cout, *scratch):
        (hb0a, hb1a, hb2a, hb0b, hb1b, hb2b, xga, xgb, cma, cmb, csa, csb, xt, fbuf, wall,
         lhs0, lhs1, lhs2, gs0, gs1, gs2, wx_ref, bias_ref, hin, sh, sc, sq, rh, rc, rq, xs, xr, xtmp, xtmp2, smask,
         lsem, ssem, rsem, xssem, xrsem) = scratch
        hbs = ((hb0a, hb1a, hb2a), (hb0b, hb1b, hb2b))
        xgs = (xga, xgb)
        cms = (cma, cmb)
        css = (csa, csb)
        lhss = (lhs0, lhs1, lhs2)
        gss = (gs0, gs1, gs2)

        ri = lax.axis_index("rows")
        ci = lax.axis_index("cols")

        def exists(k):
            dr, dc = DIRS[k]
            conds = []
            if dr < 0:
                conds.append(ri > 0)
            if dr > 0:
                conds.append(ri < row_count - 1)
            if dc < 0:
                conds.append(ci > 0)
            if dc > 0:
                conds.append(ci < col_count - 1)
            out = conds[0]
            for extra in conds[1:]:
                out = jnp.logical_and(out, extra)
            return out

        def dev(k, dst=0):
            real = jnp.logical_and(present[k], dst < nblock)
            return {"rows": jnp.where(real, ri + DIRS[k][0], partner), "cols": jnp.where(real, ci + DIRS[k][1], ci)}

        present = [exists(k) for k in range(8)]
        partner = jnp.where(lax.rem(ri, 2) == 0, ri + 1, ri - 1)
        n_row = jnp.where(ri > 0, 1, 0) + jnp.where(ri < row_count - 1, 1, 0)
        n_col = jnp.where(ci > 0, 1, 0) + jnp.where(ci < col_count - 1, 1, 0)

        p_row = jnp.where(partner > 0, 1, 0) + jnp.where(partner < row_count - 1, 1, 0)

        def pick(k, dst, real, spare):
            return jnp.where(jnp.logical_and(present[k], dst < nblock), real, spare)

        def h_addr(r, c):
            return (r + BLOCK) * pitch + COL0 + c

        def x_addr(r, c):
            return (r + ring) * pitch + COL0 + c

        cp_h = pltpu.make_async_copy(hinit, hin, lsem.at[0])
        near = BLOCK * seqs
        far = steps * seqs - near
        cp_f = pltpu.make_async_copy(frames.at[pl.ds(0, near)], fbuf.at[pl.ds(0, near)], lsem.at[1])
        cp_g = pltpu.make_async_copy(frames.at[pl.ds(near, far)], fbuf.at[pl.ds(near, far)], lsem.at[5])
        cp_w = pltpu.make_async_copy(wh_hbm, wall.at[pl.ds(0, 9 * hid), :], lsem.at[2])
        cp_c = [pltpu.make_async_copy(cinit.at[s], cms[s].at[pl.ds(ring * cols, rows * cols), :], lsem.at[3 + s]) for s in range(seqs)]
        cp_small = [pltpu.make_async_copy(wx_hbm, wx_ref, lsem.at[6]), pltpu.make_async_copy(bias_hbm, bias_ref, lsem.at[7])]
        cp_h.start()
        for s in range(seqs):
            cp_c[s].start()
        cp_f.start()
        cp_w.start()
        for cp in cp_small:
            cp.start()
        cp_g.start()

        barrier = pltpu.get_barrier_semaphore()
        for ref in (rh, rc, rq):
            ref[pl.ds(0, 2)] = jnp.zeros((2,) + ref.shape[1:], ref.dtype)
        xr[...] = jnp.zeros_like(xr)

        xlanes = xt.shape[2]

        def zero_x(i, _):
            for lane0 in (0, xlanes - 128):
                xt[i, pl.ds(COL0, cols), pl.ds(lane0, 128)] = jnp.zeros((cols, 128), F32)
            return 0

        lax.fori_loop(0, steps * seqs, zero_x, 0)
        for k in range(8):
            pl.semaphore_signal(barrier, 1, device_id=dev(k), device_id_type=MESH)
        top_ok = jnp.where(ri > 0, 1.0, 0.0).astype(F32)
        bot_ok = jnp.where(ri < row_count - 1, 1.0, 0.0).astype(F32)
        left_ok = jnp.where(ci > 0, 1.0, 0.0).astype(F32)
        right_ok = jnp.where(ci < col_count - 1, 1.0, 0.0).astype(F32)
        srow = lax.broadcasted_iota(jnp.int32, (32, hid), 0)
        rmask = jnp.where(srow < ring, top_ok, jnp.where(srow >= rows + ring, bot_ok, 1.0))
        smask[0] = rmask * left_ok
        smask[1] = rmask * right_ok

        met = (n_row + 1) * (n_col + 1) - 1
        pl.semaphore_wait(barrier, met + 8 - ((p_row + 1) * (n_col + 1) - 1))

        def msg_copies(s, k, dst):
            slot = pick(k, dst, lax.rem(dst, 2), 2 + dst)
            sem = pick(k, dst, lax.rem(dst, 2) * seqs + s, 2 * seqs + dst * seqs + s)
            if k < 4:
                pairs = ((sh.at[s, k], rh.at[slot, s, k]), (sc.at[s, k], rc.at[slot, s, k]))
            else:
                pairs = ((sq.at[s, k - 4], rq.at[slot, s, k - 4]),)
            return [
                pltpu.make_async_remote_copy(src_ref=a, dst_ref=b, send_sem=ssem.at[s], recv_sem=rsem.at[sem], device_id=dev(k, dst), device_id_type=MESH)
                for a, b in pairs
            ]

        def pack(s):
            hb = hbs[s][0]
            cm = cms[s]
            for k in range(8):
                dr, dc = DIRS[k]
                r0 = 0 if dr < 0 else rows - BLOCK
                rc0 = 0 if dr < 0 else rows - ring
                c0 = 0 if dc < 0 else cols - BLOCK
                cc0 = 0 if dc < 0 else cols - ring
                if dc == 0:
                    v = jnp.concatenate([hb[pl.ds(h_addr(r0 + i, 0), cols), :] for i in range(BLOCK)], axis=0)
                    sh[s, k, pl.ds(0, BLOCK * cols), :] = v.astype(BF16)
                    sc[s, k] = cm[pl.ds((rc0 + ring) * cols, ring * cols), :]
                elif dr == 0:
                    v = jnp.concatenate([hb[pl.ds(h_addr(0, c0 + j), rows, stride=pitch), :] for j in range(BLOCK)], axis=0)
                    sh[s, k, pl.ds(0, BLOCK * rows), :] = v.astype(BF16)
                    for j in range(ring):
                        sc[s, k, pl.ds(j * rows, rows), :] = cm[pl.ds(ring * cols + cc0 + j, rows, stride=cols), :]
                else:
                    for i in range(BLOCK):
                        sq[s, k - 4, pl.ds(i * BLOCK, BLOCK), :] = hb[pl.ds(h_addr(r0 + i, c0), BLOCK), :]
                    for j in range(ring):
                        sq[s, k - 4, pl.ds(BLOCK * BLOCK + j * ring, ring), :] = cm[pl.ds((rc0 + ring) * cols + cc0 + j, ring, stride=cols), :]

        def unpack(s, par):
            hb = hbs[s][0]
            cm = cms[s]
            cs = css[s]
            for k in range(8):
                dr, dc = DIRS[k]
                o = opposite(k)
                r0 = -BLOCK if dr < 0 else rows
                c0 = -BLOCK if dc < 0 else cols
                st0 = 0 if dc < 0 else ring
                q0 = 0 if dr < 0 else rows + ring
                if dc == 0:
                    v = rh[par, s, o, pl.ds(0, BLOCK * cols), :].astype(F32)
                    for i in range(BLOCK):
                        hb[pl.ds(h_addr(r0 + i, 0), cols), :] = v[i * cols:(i + 1) * cols]
                    cm[pl.ds(q0 * cols, ring * cols), :] = rc[par, s, o]
                elif dr == 0:
                    v = rh[par, s, o, pl.ds(0, BLOCK * rows), :].astype(F32)
                    for j in range(BLOCK):
                        hb[pl.ds(h_addr(0, c0 + j), rows, stride=pitch), :] = v[j * rows:(j + 1) * rows]
                    for j in range(ring):
                        cs[pl.ds((st0 + j) * 32 + ring, rows), :] = rc[par, s, o, pl.ds(j * rows, rows), :]
                else:
                    for i in range(BLOCK):
                        hb[pl.ds(h_addr(r0 + i, c0), BLOCK), :] = rq[par, s, o - 4, pl.ds(i * BLOCK, BLOCK), :]
                    for j in range(ring):
                        cs[pl.ds((st0 + j) * 32 + q0, ring), :] = rq[par, s, o - 4, pl.ds(BLOCK * BLOCK + j * ring, ring), :]

        def send(s, dst):
            for k in range(8):
                for cp in msg_copies(s, k, dst):
                    cp.start()

        def wait_rows(sem, n):
            pltpu.make_async_copy(cinit.at[:, pl.ds(0, n // seqs)], cout.at[:, pl.ds(0, n // seqs)], sem).wait()

        def wait_all(sem, row_size, col_size, corner_size, absent=False, more=None):
            for a in ((1, 2) if row_count > 2 else (row_count - 1,)):
                for b in ((1, 2) if col_count > 2 else (col_count - 1,)):
                    n = row_size * a + col_size * b + corner_size * a * b
                    if absent:
                        n = 2 * row_size + 2 * col_size + 4 * corner_size - n
                    cond = jnp.logical_and((p_row if absent else n_row) == a, n_col == b)
                    if n:
                        @pl.when(cond if more is None else jnp.logical_and(cond, more))
                        def _():
                            wait_rows(sem, n)

        msg_side, msg_corner = 40 + ring * cols, 16
        msg_total = 4 * (msg_side + msg_corner)

        own_lane = xrow0 * chan
        row_lanes = rows * chan

        def x_copy(first, count, k, sem):
            dr, dc = DIRS[k]
            if dc == 0:
                per = BLOCK * seqs
                src = own_lane if dr < 0 else own_lane + row_lanes - 128
                dst = own_lane + row_lanes if dr < 0 else 0
                a = xt.at[pl.ds(first * per, count * per), pl.ds(COL0, cols), pl.ds(src, 128)]
                b = xt.at[pl.ds(first * per, count * per), pl.ds(COL0, cols), pl.ds(dst, 128)]
            else:
                width = row_lanes if dr == 0 else 128
                src = row_lanes - 128 if dr > 0 else 0
                dst = {-1: own_lane + row_lanes, 0: own_lane, 1: 0}[dr]
                a = xs.at[pl.ds(first, count), 0 if dc < 0 else 1, :, pl.ds(src, width)]
                b = xr.at[pl.ds(first, count), 1 if dc < 0 else 0, :, pl.ds(dst, width)]
            return pltpu.make_async_remote_copy(
                src_ref=a, dst_ref=b, send_sem=xssem.at[sem], recv_sem=xrsem.at[sem], device_id=dev(k), device_id_type=MESH)

        x_sizes = (BLOCK * seqs * cols, 16 * row_lanes // 256, 16 * 128 // 256)

        def x_rows_of(s, q):
            w = BLOCK - q
            return s * (BLOCK * (BLOCK + 1) // 2) + sum(BLOCK - p for p in range(q)), w

        def pack_x(blk):
            for side in range(2):
                for s in range(seqs):
                    for q in range(BLOCK):
                        at, w = x_rows_of(s, q)
                        col = COL0 if side == 0 else COL0 + cols - w
                        xtmp[side, pl.ds(at, w), :] = xt[(blk * BLOCK + q) * seqs + s, pl.ds(col, w), pl.ds(own_lane, row_lanes)]
                xs[blk, side] = xtmp[side].astype(BF16)

        def unpack_x(blk):
            for side in range(2):
                v = xr[blk, side].astype(F32)
                xtmp2[side] = v
                for s in range(seqs):
                    for q in range(BLOCK):
                        at, w = x_rows_of(s, q)
                        col = COL0 - w if side == 0 else COL0 + cols
                        xt[(blk * BLOCK + q) * seqs + s, pl.ds(col, w), :] = xtmp2[side, pl.ds(at, w), :]

        def load_state(s):
            for r in range(0, rows, 2):
                v = hin[s, pl.ds(r * cols, 2 * cols), :].astype(F32)
                for i in range(2):
                    hbs[s][0][pl.ds(h_addr(r + i, 0), cols), :] = v[i * cols:(i + 1) * cols]

        cp_h.wait()
        load_state(0)
        cp_c[0].wait()
        pack(0)
        send(0, 0)

        eye = (lax.broadcasted_iota(jnp.int32, (cols, cols), 0) == lax.broadcasted_iota(jnp.int32, (cols, cols), 1)).astype(F32).astype(BF16)

        def prep_x(dst):
            for q in range(BLOCK):
                t = dst * BLOCK + q
                for s in range(seqs):
                    xt[t * seqs + s, pl.ds(COL0, cols), pl.ds(own_lane, row_lanes)] = lax.dot_general(
                        eye, fbuf[t * seqs + s], (((1,), (1,)), ((), ())), preferred_element_type=F32)


        cp_f.wait()
        prep_x(0)
        pack_x(0)

        def send_x(first, count, sem):
            for k in range(8):
                @pl.when(present[k])
                def _():
                    x_copy(first, count, k, sem).start()

        send_x(0, 1, 0)
        load_state(1)
        cp_c[1].wait()
        cp_w.wait()
        for cp in cp_small:
            cp.wait()
        wall[pl.ds(9 * hid, 3 * 128), :] = jnp.zeros((3 * 128, gates), BF16)
        for dc in range(3):
            for dr in range(3):
                wall[pl.ds(9 * hid + dc * 128 + dr * chan, chan), :] = wx_ref[dr, dc]

        cp_g.wait()

        def prep_more(blk, _):
            prep_x(blk)
            pack_x(blk)
            return 0

        lax.fori_loop(1, nblock, prep_more, 0)
        send_x(1, nblock - 1, 1)
        wait_all(xrsem.at[0], *x_sizes)
        unpack_x(0)
        lane = lax.broadcasted_iota(jnp.int32, (pitch, 128), 1)

        def build_xg(s, t, ext):
            xg = xgs[s]
            for r in range(-ext, rows + ext):
                start = r - 1 + xrow0
                g, off = divmod(start, 8)
                v = xt[t * seqs + s, :, pl.ds(g * 128, 128)]
                if off:
                    v = pltpu.roll(v, 128 - chan * off, 1)
                    if off > 5:
                        w = pltpu.roll(xt[t * seqs + s, :, pl.ds((g + 1) * 128, 128)], 128 - chan * off, 1)
                        v = jnp.where(lane < 128 - chan * off, v, w)
                xg[pl.ds(x_addr(r, -COL0), pitch), :] = v

        def build_lhs(s, j, ch):
            hb = hbs[s][j]
            xg = xgs[s]
            r0, nr, strips = chunk_list(BLOCK - 1 - j)[ch]
            lhs = lhss[ch]
            base = 32 * len(strips)
            for tap in range(12):
                for n, k in enumerate(strips):
                    if tap < 9:
                        dr, dc = tap // 3 - 1, tap % 3 - 1
                        v = hb[pl.ds(h_addr(-ring + dr, strip_cols[k] + dc), 32, stride=pitch), :]
                    else:
                        v = xg[pl.ds(x_addr(-ring, strip_cols[k] + tap - 10), 32, stride=pitch), :]
                    lhs[pl.ds(32 * n, 32), pl.ds(tap * 128, 128)] = v.astype(BF16)
                for i in range(0, nr, 2):
                    pieces = []
                    for r in range(r0 + i, min(r0 + i + 2, r0 + nr)):
                        if tap < 9:
                            dr, dc = tap // 3 - 1, tap % 3 - 1
                            pieces.append(hb[pl.ds(h_addr(r + dr, dc), cols), :])
                        else:
                            pieces.append(xg[pl.ds(x_addr(r, tap - 10), cols), :])
                    v = jnp.concatenate(pieces, axis=0) if len(pieces) > 1 else pieces[0]
                    lhs[pl.ds(base + i * cols, len(pieces) * cols), pl.ds(tap * 128, 128)] = v.astype(BF16)

        def matmul(j, ch):
            r0, nr, strips = chunk_list(BLOCK - 1 - j)[ch]
            m = -(-(32 * len(strips) + nr * cols) // 16) * 16
            gss[ch][pl.ds(0, m), :] = jnp.dot(lhss[ch][pl.ds(0, m), :], wall[...], preferred_element_type=F32)

        def cell(g_ref, m0, n, c):
            b = bias_ref[...]
            acts = []
            for q in range(4):
                g = g_ref[pl.ds(m0, n), pl.ds(q * hid, hid)] + b[:, q * hid:(q + 1) * hid]
                acts.append(jnp.tanh(g) if q == 3 else 0.5 * jnp.tanh(0.5 * g) + 0.5)
            c_new = acts[1] * c + acts[0] * acts[3]
            return acts[2] * jnp.tanh(c_new), c_new

        def elementwise(s, j, ch, t, skip=None):
            ext = BLOCK - 1 - j
            dst = hbs[s][(j + 1) % BLOCK]
            r0, nr, strips = chunk_list(ext)[ch]
            base = 32 * len(strips)
            for n, k in enumerate(strips):
                h, c_new = cell(gss[ch], 32 * n, 32, css[s][pl.ds(32 * k, 32), :])
                css[s][pl.ds(32 * k, 32), :] = c_new
                h = h * smask[0 if strip_cols[k] < 0 else 1]
                dst[pl.ds(h_addr(-ring, strip_cols[k]), 32, stride=pitch), :] = h.astype(BF16).astype(F32)
            r = r0
            while r < r0 + nr:
                inside = 0 <= r < rows
                cnt = 2 if inside else 1
                crow = (r + ring) * cols
                c_old = cms[s][pl.ds(crow, cnt * cols), :]
                h, c_new = cell(gss[ch], base + (r - r0) * cols, cnt * cols, c_old)
                if skip is not None:
                    c_new = jnp.where(skip, c_old, c_new)
                cms[s][pl.ds(crow, cnt * cols), :] = c_new
                if not inside:
                    h = h * (top_ok if r < 0 else bot_ok)
                hb16 = h.astype(BF16)
                if inside:
                    hout[t, s, pl.ds(r * cols, cnt * cols), :] = hb16
                h = hb16.astype(F32)
                for i in range(cnt):
                    new = h[i * cols:(i + 1) * cols]
                    if skip is not None:
                        new = jnp.where(skip, dst[pl.ds(h_addr(r + i, 0), cols), :], new)
                    dst[pl.ds(h_addr(r + i, 0), cols), :] = new
                r += cnt

        last = (BLOCK - 1, 2)

        def block(b, _):
            par = lax.rem(b, 2)
            for s in range(seqs):
                o = 1 - s
                wait_all(rsem.at[par * seqs + s], msg_side, msg_side, msg_corner)
                if s == 0:
                    @pl.when(b > 0)
                    def _():
                        wait_rows(ssem.at[o], msg_total)
                else:
                    wait_rows(ssem.at[o], msg_total)
                    wait_all(xrsem.at[1], *[(nblock - 1) * n for n in x_sizes], more=b == 0)
                unpack(s, par)
                build_xg(s, b * BLOCK, BLOCK - 1)
                build_lhs(s, 0, 0)
                if s == 0:
                    elementwise(o, *last, lax.rem(b * BLOCK - 1 + steps, steps), b == 0)
                    pack(o)
                    send(o, b)
                else:
                    elementwise(o, *last, b * BLOCK + BLOCK - 1)
                    pack(o)
                    send(o, b + 1)
                late = None
                for j in range(BLOCK):
                    if j > 0:
                        build_xg(s, b * BLOCK + j, BLOCK - 1 - j)
                    if s == seqs - 1 and j == BLOCK - 1:
                        unpack_x(lax.rem(b + 1, nblock))
                    for ch in range(3):
                        if j + ch > 0:
                            build_lhs(s, j, ch)
                        matmul(j, ch)
                        if late is not None:
                            elementwise(s, *late, b * BLOCK + late[0])
                        late = (j, ch)
            return 0

        lax.fori_loop(0, nblock, block, 0)
        elementwise(1, *last, steps - 1)
        wait_rows(ssem.at[0], msg_total)
        wait_rows(ssem.at[1], msg_total)
        wait_all(xssem.at[0], *x_sizes)
        wait_all(xssem.at[1], *[(nblock - 1) * n for n in x_sizes])
        for dst in range(nblock):
            for s in range(seqs):
                wait_all(rsem.at[(2 + dst) * seqs + s], msg_side, msg_side, msg_corner, absent=True)
        wait_rows(rsem.at[(2 + nblock) * seqs], msg_total)
        for s in range(seqs):
            cout[s] = cms[s][pl.ds(ring * cols, rows * cols), :]

    hbuf = pltpu.VMEM((hrows * pitch, hid), F32)
    xbuf = pltpu.VMEM((hrows * pitch, 128), F32)
    mmax = [-(-max(32 * len(chunk_list(e)[ch][2]) + chunk_list(e)[ch][1] * cols for e in range(BLOCK)) // 16) * 16 for ch in range(3)]
    scratch = (
        [hbuf] * 6 + [xbuf] * 2
        + [pltpu.VMEM(((rows + 2 * ring) * cols, hid), F32)] * 2
        + [pltpu.VMEM((nstrip * 32, hid), F32)] * 2
        + [
            pltpu.VMEM((steps * seqs, pitch, (rows + 16) * chan), F32),
            pltpu.VMEM((steps * seqs, rows * chan, cols), BF16),
            pltpu.VMEM((kdim, gates), BF16),
        ]
        + [pltpu.VMEM((mmax[ch], kdim), BF16) for ch in range(3)]
        + [pltpu.VMEM((mmax[ch], gates), F32) for ch in range(3)]
        + [
            pltpu.VMEM((3, 3, chan, gates), BF16),
            pltpu.VMEM((1, gates), F32),
            pltpu.VMEM((seqs, rows * cols, hid), BF16),
            pltpu.VMEM((seqs, 4, 80, hid), BF16),
            pltpu.VMEM((seqs, 4, ring * cols, hid), F32),
            pltpu.VMEM((seqs, 4, 16, hid), F32),
            pltpu.VMEM((3 + nblock, seqs, 4, 80, hid), BF16),
            pltpu.VMEM((3 + nblock, seqs, 4, ring * cols, hid), F32),
            pltpu.VMEM((3 + nblock, seqs, 4, 16, hid), F32),
            pltpu.VMEM((nblock, 2, 16, rows * chan), BF16),
            pltpu.VMEM((nblock, 2, 16, (rows + 16) * chan), BF16),
            pltpu.VMEM((2, 16, rows * chan), F32),
            pltpu.VMEM((2, 16, (rows + 16) * chan), F32),
            pltpu.VMEM((2, 32, hid), F32),
            pltpu.SemaphoreType.DMA((8,)),
            pltpu.SemaphoreType.DMA((seqs,)),
            pltpu.SemaphoreType.DMA(((3 + nblock) * seqs,)),
            pltpu.SemaphoreType.DMA((2,)),
            pltpu.SemaphoreType.DMA((2,)),
        ]
    )
    return kernel, scratch


def solution(mesh):
    row_count = mesh.shape["rows"]
    col_count = mesh.shape["cols"]
    frame_spec = P(None, "batch", "rows", "cols", None)
    state_spec = P("batch", "rows", "cols", None)

    def local_run(frames, w_x, w_h, gate_bias, h_init, c_init):
        steps, seqs, rows, cols, chan = frames.shape
        hid = h_init.shape[-1]
        gates = 4 * hid
        kernel, scratch = make_kernel(steps, seqs, rows, cols, chan, hid, row_count, col_count)
        hbm = pl.BlockSpec(memory_space=pltpu.HBM)
        vmem = pl.BlockSpec(memory_space=pltpu.VMEM)
        ft = frames.transpose(0, 1, 2, 4, 3).reshape(steps * seqs, rows * chan, cols)
        all_hidden, cell_last = pl.pallas_call(
            kernel,
            out_shape=(
                pltpu.VMEM((steps, seqs, rows * cols, hid), BF16),
                pltpu.VMEM((seqs, rows * cols, hid), F32),
            ),
            in_specs=[hbm] * 6,
            out_specs=(vmem, vmem),
            scratch_shapes=scratch,
            compiler_params=pltpu.CompilerParams(collective_id=0, has_side_effects=True, vmem_limit_bytes=44 * 1024 * 1024),
        )(
            *[
                pltpu.with_memory_space_constraint(x, pltpu.HBM)
                for x in (
                    ft, w_x, w_h.reshape(9 * hid, gates), gate_bias.reshape(1, gates),
                    h_init.reshape(seqs, rows * cols, hid), c_init.reshape(seqs, rows * cols, hid),
                )
            ]
        )
        return all_hidden.reshape(steps, seqs, rows, cols, hid), cell_last.reshape(seqs, rows, cols, hid)

    return jax.shard_map(local_run, mesh=mesh, in_specs=(frame_spec, P(), P(), P(), state_spec, state_spec), out_specs=(frame_spec, state_spec), check_vma=False)
```

```python
import jax
import jax.numpy as jnp
from jax import lax
from jax.experimental import pallas as pl
from jax.experimental.pallas import tpu as pltpu
from jax.sharding import PartitionSpec as P

BLOCK = 3
COL0 = 8
DIRS = ((-1, 0), (1, 0), (0, -1), (0, 1), (-1, -1), (-1, 1), (1, -1), (1, 1))
MESH = pl.DeviceIdType.MESH
F32 = jnp.float32
BF16 = jnp.bfloat16


def opposite(k):
    return DIRS.index((-DIRS[k][0], -DIRS[k][1]))


def make_kernel(steps, seqs, rows, cols, chan, hid, row_count, col_count):
    nblock = steps // BLOCK
    pitch = cols + 16
    hrows = rows + 2 * BLOCK + 6
    ring = BLOCK - 1
    xrow0 = 8
    nstrip = 2 * ring
    gates = 4 * hid
    kdim = 9 * hid + 3 * 128
    strip_cols = tuple(range(-ring, 0)) + tuple(range(cols, cols + ring))
    third = rows // 3

    def chunk_list(ext):
        own = [c for c in range(nstrip) if -ext <= strip_cols[c] < cols + ext]
        return (
            (-ext, third + ext, ()),
            (third, third, tuple(own)),
            (2 * third, third + ext, ()),
        )

    def kernel(frames, wx_hbm, wh_hbm, bias_hbm, hinit, cinit, hout, cout, *scratch):
        (hb0a, hb1a, hb2a, hb0b, hb1b, hb2b, xga, xgb, cma, cmb, csa, csb, xt, fbuf, wall,
         lhs0, lhs1, lhs2, gs0, gs1, gs2, wx_ref, bias_ref, hin, sh, sc, sq, rh, rc, rq, xs, xr, xtmp, xtmp2, smask,
         lsem, ssem, rsem, xssem, xrsem) = scratch
        hbs = ((hb0a, hb1a, hb2a), (hb0b, hb1b, hb2b))
        xgs = (xga, xgb)
        cms = (cma, cmb)
        css = (csa, csb)
        lhss = (lhs0, lhs1, lhs2)
        gss = (gs0, gs1, gs2)

        ri = lax.axis_index("rows")
        ci = lax.axis_index("cols")

        def exists(k):
            dr, dc = DIRS[k]
            conds = []
            if dr < 0:
                conds.append(ri > 0)
            if dr > 0:
                conds.append(ri < row_count - 1)
            if dc < 0:
                conds.append(ci > 0)
            if dc > 0:
                conds.append(ci < col_count - 1)
            out = conds[0]
            for extra in conds[1:]:
                out = jnp.logical_and(out, extra)
            return out

        def dev(k):
            return {"rows": jnp.where(present[k], ri + DIRS[k][0], partner), "cols": jnp.where(present[k], ci + DIRS[k][1], ci)}

        present = [exists(k) for k in range(8)]
        partner = jnp.where(lax.rem(ri, 2) == 0, ri + 1, ri - 1)
        n_row = jnp.where(ri > 0, 1, 0) + jnp.where(ri < row_count - 1, 1, 0)
        n_col = jnp.where(ci > 0, 1, 0) + jnp.where(ci < col_count - 1, 1, 0)

        p_row = jnp.where(partner > 0, 1, 0) + jnp.where(partner < row_count - 1, 1, 0)

        def pick(k, real, spare):
            return jnp.where(present[k], real, spare)

        def h_addr(r, c):
            return (r + BLOCK) * pitch + COL0 + c

        def x_addr(r, c):
            return (r + ring) * pitch + COL0 + c

        cp_h = pltpu.make_async_copy(hinit, hin, lsem.at[0])
        near = BLOCK * seqs
        far = steps * seqs - near
        cp_f = pltpu.make_async_copy(frames.at[pl.ds(0, near)], fbuf.at[pl.ds(0, near)], lsem.at[1])
        cp_g = pltpu.make_async_copy(frames.at[pl.ds(near, far)], fbuf.at[pl.ds(near, far)], lsem.at[5])
        cp_w = pltpu.make_async_copy(wh_hbm, wall.at[pl.ds(0, 9 * hid), :], lsem.at[2])
        cp_c = [pltpu.make_async_copy(cinit.at[s], cms[s].at[pl.ds(ring * cols, rows * cols), :], lsem.at[3 + s]) for s in range(seqs)]
        cp_small = [pltpu.make_async_copy(wx_hbm, wx_ref, lsem.at[6]), pltpu.make_async_copy(bias_hbm, bias_ref, lsem.at[7])]
        cp_h.start()
        for s in range(seqs):
            cp_c[s].start()
        cp_f.start()
        cp_w.start()
        for cp in cp_small:
            cp.start()
        cp_g.start()

        barrier = pltpu.get_barrier_semaphore()
        for k in range(8):
            pl.semaphore_signal(barrier, 1, device_id=dev(k), device_id_type=MESH)

        top_ok = jnp.where(ri > 0, 1.0, 0.0).astype(F32)
        bot_ok = jnp.where(ri < row_count - 1, 1.0, 0.0).astype(F32)
        left_ok = jnp.where(ci > 0, 1.0, 0.0).astype(F32)
        right_ok = jnp.where(ci < col_count - 1, 1.0, 0.0).astype(F32)
        srow = lax.broadcasted_iota(jnp.int32, (32, hid), 0)
        rmask = jnp.where(srow < ring, top_ok, jnp.where(srow >= rows + ring, bot_ok, 1.0))
        smask[0] = rmask * left_ok
        smask[1] = rmask * right_ok

        met = (n_row + 1) * (n_col + 1) - 1
        pl.semaphore_wait(barrier, met + 8 - ((p_row + 1) * (n_col + 1) - 1))

        def msg_copies(s, k, dst):
            slot = pick(k, lax.rem(dst, 2), 2 + dst)
            sem = pick(k, lax.rem(dst, 2) * seqs + s, 2 * seqs + dst * seqs + s)
            if k < 4:
                pairs = ((sh.at[s, k], rh.at[slot, s, k]), (sc.at[s, k], rc.at[slot, s, k]))
            else:
                pairs = ((sq.at[s, k - 4], rq.at[slot, s, k - 4]),)
            return [
                pltpu.make_async_remote_copy(src_ref=a, dst_ref=b, send_sem=ssem.at[s], recv_sem=rsem.at[sem], device_id=dev(k), device_id_type=MESH)
                for a, b in pairs
            ]

        def pack(s):
            hb = hbs[s][0]
            cm = cms[s]
            for k in range(8):
                dr, dc = DIRS[k]
                r0 = 0 if dr < 0 else rows - BLOCK
                rc0 = 0 if dr < 0 else rows - ring
                c0 = 0 if dc < 0 else cols - BLOCK
                cc0 = 0 if dc < 0 else cols - ring
                if dc == 0:
                    v = jnp.concatenate([hb[pl.ds(h_addr(r0 + i, 0), cols), :] for i in range(BLOCK)], axis=0)
                    sh[s, k, pl.ds(0, BLOCK * cols), :] = v.astype(BF16)
                    sc[s, k] = cm[pl.ds((rc0 + ring) * cols, ring * cols), :]
                elif dr == 0:
                    v = jnp.concatenate([hb[pl.ds(h_addr(0, c0 + j), rows, stride=pitch), :] for j in range(BLOCK)], axis=0)
                    sh[s, k, pl.ds(0, BLOCK * rows), :] = v.astype(BF16)
                    for j in range(ring):
                        sc[s, k, pl.ds(j * rows, rows), :] = cm[pl.ds(ring * cols + cc0 + j, rows, stride=cols), :]
                else:
                    for i in range(BLOCK):
                        sq[s, k - 4, pl.ds(i * BLOCK, BLOCK), :] = hb[pl.ds(h_addr(r0 + i, c0), BLOCK), :]
                    for j in range(ring):
                        sq[s, k - 4, pl.ds(BLOCK * BLOCK + j * ring, ring), :] = cm[pl.ds((rc0 + ring) * cols + cc0 + j, ring, stride=cols), :]

        def unpack(s, par):
            hb = hbs[s][0]
            cm = cms[s]
            cs = css[s]
            for k in range(8):
                dr, dc = DIRS[k]
                o = opposite(k)
                r0 = -BLOCK if dr < 0 else rows
                c0 = -BLOCK if dc < 0 else cols
                st0 = 0 if dc < 0 else ring
                q0 = 0 if dr < 0 else rows + ring
                if dc == 0:
                    v = rh[par, s, o, pl.ds(0, BLOCK * cols), :].astype(F32)
                    for i in range(BLOCK):
                        hb[pl.ds(h_addr(r0 + i, 0), cols), :] = v[i * cols:(i + 1) * cols]
                    cm[pl.ds(q0 * cols, ring * cols), :] = rc[par, s, o]
                elif dr == 0:
                    v = rh[par, s, o, pl.ds(0, BLOCK * rows), :].astype(F32)
                    for j in range(BLOCK):
                        hb[pl.ds(h_addr(0, c0 + j), rows, stride=pitch), :] = v[j * rows:(j + 1) * rows]
                    for j in range(ring):
                        cs[pl.ds((st0 + j) * 32 + ring, rows), :] = rc[par, s, o, pl.ds(j * rows, rows), :]
                else:
                    for i in range(BLOCK):
                        hb[pl.ds(h_addr(r0 + i, c0), BLOCK), :] = rq[par, s, o - 4, pl.ds(i * BLOCK, BLOCK), :]
                    for j in range(ring):
                        cs[pl.ds((st0 + j) * 32 + q0, ring), :] = rq[par, s, o - 4, pl.ds(BLOCK * BLOCK + j * ring, ring), :]

        def send(s, dst):
            for k in (4, 5, 6, 7):
                msg_copies(s, k, dst)[0].start()
            for n in range(2):
                for k in (2, 3, 0, 1):
                    msg_copies(s, k, dst)[n].start()

        def wait_rows(sem, n):
            pltpu.make_async_copy(cinit.at[:, pl.ds(0, n // seqs)], cout.at[:, pl.ds(0, n // seqs)], sem).wait()

        def wait_all(sem, row_size, col_size, corner_size, absent=False, more=None):
            for a in ((1, 2) if row_count > 2 else (row_count - 1,)):
                for b in ((1, 2) if col_count > 2 else (col_count - 1,)):
                    n = row_size * a + col_size * b + corner_size * a * b
                    if absent:
                        n = 2 * row_size + 2 * col_size + 4 * corner_size - n
                    cond = jnp.logical_and((p_row if absent else n_row) == a, n_col == b)
                    if n:
                        @pl.when(cond if more is None else jnp.logical_and(cond, more))
                        def _():
                            wait_rows(sem, n)

        msg_side, msg_corner = 40 + ring * cols, 16
        msg_total = 4 * (msg_side + msg_corner)

        own_lane = xrow0 * chan
        row_lanes = rows * chan

        def x_copy(first, count, k, sem):
            dr, dc = DIRS[k]
            if dc == 0:
                per = BLOCK * seqs
                src = own_lane if dr < 0 else own_lane + row_lanes - 128
                dst = own_lane + row_lanes if dr < 0 else 0
                a = xt.at[pl.ds(first * per, count * per), pl.ds(COL0, cols), pl.ds(src, 128)]
                b = xt.at[pl.ds(first * per, count * per), pl.ds(COL0, cols), pl.ds(dst, 128)]
            else:
                width = row_lanes if dr == 0 else 128
                src = row_lanes - 128 if dr > 0 else 0
                dst = {-1: own_lane + row_lanes, 0: own_lane, 1: 0}[dr]
                a = xs.at[pl.ds(first, count), 0 if dc < 0 else 1, :, pl.ds(src, width)]
                b = xr.at[pl.ds(first, count), 1 if dc < 0 else 0, :, pl.ds(dst, width)]
            return pltpu.make_async_remote_copy(
                src_ref=a, dst_ref=b, send_sem=xssem.at[sem], recv_sem=xrsem.at[sem], device_id=dev(k), device_id_type=MESH)

        x_sizes = (BLOCK * seqs * cols, 16 * row_lanes // 256, 16 * 128 // 256)

        def x_rows_of(s, q):
            w = BLOCK - q
            return s * (BLOCK * (BLOCK + 1) // 2) + sum(BLOCK - p for p in range(q)), w

        def pack_x(blk):
            for side in range(2):
                for s in range(seqs):
                    for q in range(BLOCK):
                        at, w = x_rows_of(s, q)
                        col = COL0 if side == 0 else COL0 + cols - w
                        xtmp[side, pl.ds(at, w), :] = xt[(blk * BLOCK + q) * seqs + s, pl.ds(col, w), pl.ds(own_lane, row_lanes)]
                xs[blk, side] = xtmp[side].astype(BF16)

        def unpack_x(blk):
            for side in range(2):
                v = xr[blk, side].astype(F32)
                xtmp2[side] = v
                for s in range(seqs):
                    for q in range(BLOCK):
                        at, w = x_rows_of(s, q)
                        col = COL0 - w if side == 0 else COL0 + cols
                        xt[(blk * BLOCK + q) * seqs + s, pl.ds(col, w), :] = xtmp2[side, pl.ds(at, w), :]

        def load_state(s):
            for r in range(0, rows, 2):
                v = hin[s, pl.ds(r * cols, 2 * cols), :].astype(F32)
                for i in range(2):
                    hbs[s][0][pl.ds(h_addr(r + i, 0), cols), :] = v[i * cols:(i + 1) * cols]

        cp_h.wait()
        load_state(0)
        cp_c[0].wait()
        pack(0)
        send(0, 0)

        eye = (lax.broadcasted_iota(jnp.int32, (cols, cols), 0) == lax.broadcasted_iota(jnp.int32, (cols, cols), 1)).astype(F32).astype(BF16)

        def prep_x(dst):
            for q in range(BLOCK):
                t = dst * BLOCK + q
                for s in range(seqs):
                    xt[t * seqs + s, pl.ds(COL0, cols), pl.ds(own_lane, row_lanes)] = lax.dot_general(
                        eye, fbuf[t * seqs + s], (((1,), (1,)), ((), ())), preferred_element_type=F32)


        cp_f.wait()
        prep_x(0)
        pack_x(0)

        def send_x(first, count, sem):
            for k in range(8):
                @pl.when(present[k])
                def _():
                    x_copy(first, count, k, sem).start()

        send_x(0, 1, 0)
        load_state(1)
        cp_c[1].wait()
        pack(1)
        send(1, 0)
        cp_w.wait()
        for cp in cp_small:
            cp.wait()
        wall[pl.ds(9 * hid, 3 * 128), :] = jnp.zeros((3 * 128, gates), BF16)
        for dc in range(3):
            for dr in range(3):
                wall[pl.ds(9 * hid + dc * 128 + dr * chan, chan), :] = wx_ref[dr, dc]

        cp_g.wait()

        def prep_more(blk, _):
            prep_x(blk)
            pack_x(blk)
            return 0

        lax.fori_loop(1, nblock, prep_more, 0)
        send_x(1, nblock - 1, 1)
        for k in range(8):
            o = opposite(k)

            @pl.when(jnp.logical_not(present[k]))
            def _():
                for par in range(2):
                    for s in range(seqs):
                        if k < 4:
                            rh[par, s, o] = jnp.zeros(rh.shape[3:], BF16)
                            rc[par, s, o] = jnp.zeros(rc.shape[3:], F32)
                        else:
                            rq[par, s, o - 4] = jnp.zeros(rq.shape[3:], F32)
                dr, dc = DIRS[k]
                if dc == 0:
                    lane0 = 0 if dr < 0 else own_lane + row_lanes

                    def zero_x(i, _):
                        xt[i, pl.ds(COL0, cols), pl.ds(lane0, 128)] = jnp.zeros((cols, 128), F32)
                        return 0

                    lax.fori_loop(0, steps * seqs, zero_x, 0)
                else:
                    lane0 = {-1: 0, 0: own_lane, 1: own_lane + row_lanes}[dr]
                    n = row_lanes if dr == 0 else 128
                    xr[:, 0 if dc < 0 else 1, :, pl.ds(lane0, n)] = jnp.zeros((nblock, 16, n), BF16)

        wait_all(xrsem.at[0], *x_sizes)
        unpack_x(0)
        lane = lax.broadcasted_iota(jnp.int32, (pitch, 128), 1)

        def build_xg(s, t, ext):
            xg = xgs[s]
            for r in range(-ext, rows + ext):
                start = r - 1 + xrow0
                g, off = divmod(start, 8)
                v = xt[t * seqs + s, :, pl.ds(g * 128, 128)]
                if off:
                    v = pltpu.roll(v, 128 - chan * off, 1)
                    if off > 5:
                        w = pltpu.roll(xt[t * seqs + s, :, pl.ds((g + 1) * 128, 128)], 128 - chan * off, 1)
                        v = jnp.where(lane < 128 - chan * off, v, w)
                xg[pl.ds(x_addr(r, -COL0), pitch), :] = v

        def build_lhs(s, j, ch, taps=tuple(range(12))):
            hb = hbs[s][j]
            xg = xgs[s]
            r0, nr, strips = chunk_list(BLOCK - 1 - j)[ch]
            lhs = lhss[ch]
            base = 32 * len(strips)
            for tap in taps:
                for n, k in enumerate(strips):
                    if tap < 9:
                        dr, dc = tap // 3 - 1, tap % 3 - 1
                        v = hb[pl.ds(h_addr(-ring + dr, strip_cols[k] + dc), 32, stride=pitch), :]
                    else:
                        v = xg[pl.ds(x_addr(-ring, strip_cols[k] + tap - 10), 32, stride=pitch), :]
                    lhs[pl.ds(32 * n, 32), pl.ds(tap * 128, 128)] = v.astype(BF16)

            def rows_of(ref, addr, r, cnt, dc):
                v = [ref[pl.ds(addr(r + i, dc), cols), :] for i in range(cnt)]
                return (jnp.concatenate(v, axis=0) if cnt > 1 else v[0]).astype(BF16)

            def put(tap, i, cnt, v):
                lhs[pl.ds(base + i * cols, cnt * cols), pl.ds(tap * 128, 128)] = v

            pairs = [(i, min(2, nr - i)) for i in range(0, nr, 2)]
            for dc in (-1, 0, 1):
                if dc + 10 in taps:
                    for i, cnt in pairs:
                        put(dc + 10, i, cnt, rows_of(xg, x_addr, r0 + i, cnt, dc))
                if dc + 1 in taps:
                    for i, cnt in pairs:
                        put(dc + 4, i, cnt, rows_of(hb, h_addr, r0 + i, cnt, dc))
                        if cnt == 2:
                            v = rows_of(hb, h_addr, r0 + i - 1, 2, dc)
                            put(dc + 1, i, 2, v)
                            if i:
                                put(dc + 7, i - 2, 2, v)
                        else:
                            v = rows_of(hb, h_addr, r0 + i - 1, 2, dc)
                            put(dc + 7, i - 2, 2, v)
                            put(dc + 1, i, 1, rows_of(hb, h_addr, r0 + i - 1, 1, dc))
                    i, cnt = pairs[-1]
                    put(dc + 7, i, cnt, rows_of(hb, h_addr, r0 + i + 1, cnt, dc))

        def matmul(j, ch):
            r0, nr, strips = chunk_list(BLOCK - 1 - j)[ch]
            m = -(-(32 * len(strips) + nr * cols) // 16) * 16
            gss[ch][pl.ds(0, m), :] = jnp.dot(lhss[ch][pl.ds(0, m), :], wall[...], preferred_element_type=F32)

        def cell(g_ref, m0, n, c):
            b = bias_ref[...]
            acts = []
            for q in range(4):
                g = g_ref[pl.ds(m0, n), pl.ds(q * hid, hid)] + b[:, q * hid:(q + 1) * hid]
                acts.append(jnp.tanh(g) if q == 3 else 0.5 * jnp.tanh(0.5 * g) + 0.5)
            c_new = acts[1] * c + acts[0] * acts[3]
            return acts[2] * jnp.tanh(c_new), c_new

        def elementwise(s, j, ch, t):
            ext = BLOCK - 1 - j
            dst = hbs[s][(j + 1) % BLOCK]
            r0, nr, strips = chunk_list(ext)[ch]
            base = 32 * len(strips)
            for n, k in enumerate(strips):
                h, c_new = cell(gss[ch], 32 * n, 32, css[s][pl.ds(32 * k, 32), :])
                css[s][pl.ds(32 * k, 32), :] = c_new
                h = h * smask[0 if strip_cols[k] < 0 else 1]
                dst[pl.ds(h_addr(-ring, strip_cols[k]), 32, stride=pitch), :] = h.astype(BF16).astype(F32)
            r = r0
            while r < r0 + nr:
                inside = 0 <= r < rows
                cnt = 2 if inside else 1
                crow = (r + ring) * cols
                c_old = cms[s][pl.ds(crow, cnt * cols), :]
                h, c_new = cell(gss[ch], base + (r - r0) * cols, cnt * cols, c_old)
                cms[s][pl.ds(crow, cnt * cols), :] = c_new
                if not inside:
                    h = h * (top_ok if r < 0 else bot_ok)
                hb16 = h.astype(BF16)
                if inside:
                    hout[t, s, pl.ds(r * cols, cnt * cols), :] = hb16
                h = hb16.astype(F32)
                for i in range(cnt):
                    dst[pl.ds(h_addr(r + i, 0), cols), :] = h[i * cols:(i + 1) * cols]
                r += cnt

        def block(b, _):
            par = lax.rem(b, 2)
            for s in range(seqs):
                o = 1 - s
                wait_all(rsem.at[par * seqs + s], msg_side, msg_side, msg_corner)
                wait_rows(ssem.at[s], msg_total)
                if s > 0:
                    wait_all(xrsem.at[1], *[(nblock - 1) * n for n in x_sizes], more=b == 0)
                unpack(s, par)
                build_lhs(s, 0, 0, tuple(range(9)))
                late = None
                for j in range(BLOCK):
                    if j > 0:
                        build_xg(s, b * BLOCK + j, BLOCK - 1 - j)
                    if s == seqs - 1 and j == BLOCK - 1:
                        unpack_x(lax.rem(b + 1, nblock))
                    for ch in range(3):
                        if j + ch > 0:
                            build_lhs(s, j, ch)
                        matmul(j, ch)
                        if late is not None:
                            elementwise(s, *late, b * BLOCK + late[0])
                        late = (j, ch)
                    if j == BLOCK - 1:
                        build_xg(o, lax.rem((b + s) * BLOCK, steps), BLOCK - 1)
                        build_lhs(o, 0, 0, (9, 10, 11))
                elementwise(s, *late, b * BLOCK + late[0])

                @pl.when(b < nblock - 1)
                def _():
                    pack(s)
                    send(s, b + 1)
            return 0

        build_xg(0, 0, BLOCK - 1)
        build_lhs(0, 0, 0, (9, 10, 11))
        lax.fori_loop(0, nblock, block, 0)
        wait_all(xssem.at[0], *x_sizes)
        wait_all(xssem.at[1], *[(nblock - 1) * n for n in x_sizes])
        for dst in range(nblock):
            for s in range(seqs):
                wait_all(rsem.at[(2 + dst) * seqs + s], msg_side, msg_side, msg_corner, absent=True)
        for s in range(seqs):
            cout[s] = cms[s][pl.ds(ring * cols, rows * cols), :]

    hbuf = pltpu.VMEM((hrows * pitch, hid), F32)
    xbuf = pltpu.VMEM((hrows * pitch, 128), F32)
    mmax = [-(-max(32 * len(chunk_list(e)[ch][2]) + chunk_list(e)[ch][1] * cols for e in range(BLOCK)) // 16) * 16 for ch in range(3)]
    scratch = (
        [hbuf] * 6 + [xbuf] * 2
        + [pltpu.VMEM(((rows + 2 * ring) * cols, hid), F32)] * 2
        + [pltpu.VMEM((nstrip * 32, hid), F32)] * 2
        + [
            pltpu.VMEM((steps * seqs, pitch, (rows + 16) * chan), F32),
            pltpu.VMEM((steps * seqs, rows * chan, cols), BF16),
            pltpu.VMEM((kdim, gates), BF16),
        ]
        + [pltpu.VMEM((mmax[ch], kdim), BF16) for ch in range(3)]
        + [pltpu.VMEM((mmax[ch], gates), F32) for ch in range(3)]
        + [
            pltpu.VMEM((3, 3, chan, gates), BF16),
            pltpu.VMEM((1, gates), F32),
            pltpu.VMEM((seqs, rows * cols, hid), BF16),
            pltpu.VMEM((seqs, 4, 80, hid), BF16),
            pltpu.VMEM((seqs, 4, ring * cols, hid), F32),
            pltpu.VMEM((seqs, 4, 16, hid), F32),
            pltpu.VMEM((2 + nblock, seqs, 4, 80, hid), BF16),
            pltpu.VMEM((2 + nblock, seqs, 4, ring * cols, hid), F32),
            pltpu.VMEM((2 + nblock, seqs, 4, 16, hid), F32),
            pltpu.VMEM((nblock, 2, 16, rows * chan), BF16),
            pltpu.VMEM((nblock, 2, 16, (rows + 16) * chan), BF16),
            pltpu.VMEM((2, 16, rows * chan), F32),
            pltpu.VMEM((2, 16, (rows + 16) * chan), F32),
            pltpu.VMEM((2, 32, hid), F32),
            pltpu.SemaphoreType.DMA((8,)),
            pltpu.SemaphoreType.DMA((seqs,)),
            pltpu.SemaphoreType.DMA(((2 + nblock) * seqs,)),
            pltpu.SemaphoreType.DMA((2,)),
            pltpu.SemaphoreType.DMA((2,)),
        ]
    )
    return kernel, scratch


def solution(mesh):
    row_count = mesh.shape["rows"]
    col_count = mesh.shape["cols"]
    frame_spec = P(None, "batch", "rows", "cols", None)
    state_spec = P("batch", "rows", "cols", None)

    def local_run(frames, w_x, w_h, gate_bias, h_init, c_init):
        steps, seqs, rows, cols, chan = frames.shape
        hid = h_init.shape[-1]
        gates = 4 * hid
        kernel, scratch = make_kernel(steps, seqs, rows, cols, chan, hid, row_count, col_count)
        hbm = pl.BlockSpec(memory_space=pltpu.HBM)
        vmem = pl.BlockSpec(memory_space=pltpu.VMEM)
        ft = frames.transpose(0, 1, 2, 4, 3).reshape(steps * seqs, rows * chan, cols)
        all_hidden, cell_last = pl.pallas_call(
            kernel,
            out_shape=(
                pltpu.VMEM((steps, seqs, rows * cols, hid), BF16),
                pltpu.VMEM((seqs, rows * cols, hid), F32),
            ),
            in_specs=[hbm] * 6,
            out_specs=(vmem, vmem),
            scratch_shapes=scratch,
            compiler_params=pltpu.CompilerParams(collective_id=0, has_side_effects=True, vmem_limit_bytes=44 * 1024 * 1024),
        )(
            *[
                pltpu.with_memory_space_constraint(x, pltpu.HBM)
                for x in (
                    ft, w_x, w_h.reshape(9 * hid, gates), gate_bias.reshape(1, gates),
                    h_init.reshape(seqs, rows * cols, hid), c_init.reshape(seqs, rows * cols, hid),
                )
            ]
        )
        return all_hidden.reshape(steps, seqs, rows, cols, hid), cell_last.reshape(seqs, rows, cols, hid)

    return jax.shard_map(local_run, mesh=mesh, in_specs=(frame_spec, P(), P(), P(), state_spec, state_spec), out_specs=(frame_spec, state_spec), check_vma=False)
```

```python
import jax
import jax.numpy as jnp
from jax import lax
from jax.experimental import pallas as pl
from jax.experimental.pallas import tpu as pltpu
from jax.sharding import PartitionSpec as P

BLOCK = 3
COL0 = 8
DIRS = ((-1, 0), (1, 0), (0, -1), (0, 1), (-1, -1), (-1, 1), (1, -1), (1, 1))
MESH = pl.DeviceIdType.MESH
F32 = jnp.float32
BF16 = jnp.bfloat16


def opposite(k):
    return DIRS.index((-DIRS[k][0], -DIRS[k][1]))


def make_kernel(steps, seqs, rows, cols, chan, hid, row_count, col_count):
    nblock = steps // BLOCK
    pitch = cols + 16
    hrows = rows + 2 * BLOCK + 6
    ring = BLOCK - 1
    xrow0 = 8
    nstrip = 2 * ring
    gates = 4 * hid
    kdim = 9 * hid + 3 * 128
    strip_cols = tuple(range(-ring, 0)) + tuple(range(cols, cols + ring))
    third = rows // 3

    def chunk_list(ext):
        own = [c for c in range(nstrip) if -ext <= strip_cols[c] < cols + ext]
        return (
            (-ext, third + ext, ()),
            (third, third, tuple(own)),
            (2 * third, third + ext, ()),
        )

    def kernel(frames, wx_hbm, wh_hbm, bias_hbm, hinit, cinit, hout, cout, *scratch):
        (hb0a, hb1a, hb2a, hb0b, hb1b, hb2b, xga, xgb, cma, cmb, csa, csb, xt, fbuf, wall,
         lhs0, lhs1, lhs2, gs0, gs1, gs2, wx_ref, bias_ref, hin, sh, sc, sq, rh, rc, rq, xs, xr, xtmp, xtmp2, smask,
         lsem, ssem, rsem, xssem, xrsem) = scratch
        hbs = ((hb0a, hb1a, hb2a), (hb0b, hb1b, hb2b))
        xgs = (xga, xgb)
        cms = (cma, cmb)
        css = (csa, csb)
        lhss = (lhs0, lhs1, lhs2)
        gss = (gs0, gs1, gs2)

        ri = lax.axis_index("rows")
        ci = lax.axis_index("cols")

        def exists(k):
            dr, dc = DIRS[k]
            conds = []
            if dr < 0:
                conds.append(ri > 0)
            if dr > 0:
                conds.append(ri < row_count - 1)
            if dc < 0:
                conds.append(ci > 0)
            if dc > 0:
                conds.append(ci < col_count - 1)
            out = conds[0]
            for extra in conds[1:]:
                out = jnp.logical_and(out, extra)
            return out

        def dev(k):
            return {"rows": jnp.where(present[k], ri + DIRS[k][0], partner), "cols": jnp.where(present[k], ci + DIRS[k][1], ci)}

        present = [exists(k) for k in range(8)]
        partner = jnp.where(lax.rem(ri, 2) == 0, ri + 1, ri - 1)
        n_row = jnp.where(ri > 0, 1, 0) + jnp.where(ri < row_count - 1, 1, 0)
        n_col = jnp.where(ci > 0, 1, 0) + jnp.where(ci < col_count - 1, 1, 0)

        p_row = jnp.where(partner > 0, 1, 0) + jnp.where(partner < row_count - 1, 1, 0)

        def pick(k, real, spare):
            return jnp.where(present[k], real, spare)

        def h_addr(r, c):
            return (r + BLOCK) * pitch + COL0 + c

        def x_addr(r, c):
            return (r + ring) * pitch + COL0 + c

        cp_h = pltpu.make_async_copy(hinit, hin, lsem.at[0])
        near = BLOCK * seqs
        far = steps * seqs - near
        cp_f = pltpu.make_async_copy(frames.at[pl.ds(0, near)], fbuf.at[pl.ds(0, near)], lsem.at[1])
        cp_g = pltpu.make_async_copy(frames.at[pl.ds(near, far)], fbuf.at[pl.ds(near, far)], lsem.at[5])
        cp_w = pltpu.make_async_copy(wh_hbm, wall.at[pl.ds(0, 9 * hid), :], lsem.at[2])
        cp_c = [pltpu.make_async_copy(cinit.at[s], cms[s].at[pl.ds(ring * cols, rows * cols), :], lsem.at[3 + s]) for s in range(seqs)]
        cp_small = [pltpu.make_async_copy(wx_hbm, wx_ref, lsem.at[6]), pltpu.make_async_copy(bias_hbm, bias_ref, lsem.at[7])]
        cp_h.start()
        for s in range(seqs):
            cp_c[s].start()
        cp_f.start()
        cp_w.start()
        for cp in cp_small:
            cp.start()
        cp_g.start()

        barrier = pltpu.get_barrier_semaphore()
        for k in range(8):
            pl.semaphore_signal(barrier, 1, device_id=dev(k), device_id_type=MESH)

        top_ok = jnp.where(ri > 0, 1.0, 0.0).astype(F32)
        bot_ok = jnp.where(ri < row_count - 1, 1.0, 0.0).astype(F32)
        left_ok = jnp.where(ci > 0, 1.0, 0.0).astype(F32)
        right_ok = jnp.where(ci < col_count - 1, 1.0, 0.0).astype(F32)
        srow = lax.broadcasted_iota(jnp.int32, (32, hid), 0)
        rmask = jnp.where(srow < ring, top_ok, jnp.where(srow >= rows + ring, bot_ok, 1.0))
        smask[0] = rmask * left_ok
        smask[1] = rmask * right_ok

        def msg_copies(s, k, dst):
            slot = pick(k, lax.rem(dst, 2), 2 + dst)
            sem = pick(k, lax.rem(dst, 2) * seqs + s, 2 * seqs + dst * seqs + s)
            if k < 4:
                pairs = ((sh.at[s, k], rh.at[slot, s, k]), (sc.at[s, k], rc.at[slot, s, k]))
            else:
                pairs = ((sq.at[s, k - 4], rq.at[slot, s, k - 4]),)
            return [
                pltpu.make_async_remote_copy(src_ref=a, dst_ref=b, send_sem=ssem.at[s], recv_sem=rsem.at[sem], device_id=dev(k), device_id_type=MESH)
                for a, b in pairs
            ]

        def pack(s):
            hb = hbs[s][0]
            cm = cms[s]
            for k in range(8):
                dr, dc = DIRS[k]
                r0 = 0 if dr < 0 else rows - BLOCK
                rc0 = 0 if dr < 0 else rows - ring
                c0 = 0 if dc < 0 else cols - BLOCK
                cc0 = 0 if dc < 0 else cols - ring
                if dc == 0:
                    v = jnp.concatenate([hb[pl.ds(h_addr(r0 + i, 0), cols), :] for i in range(BLOCK)], axis=0)
                    sh[s, k, pl.ds(0, BLOCK * cols), :] = v.astype(BF16)
                    sc[s, k] = cm[pl.ds((rc0 + ring) * cols, ring * cols), :]
                elif dr == 0:
                    v = jnp.concatenate([hb[pl.ds(h_addr(0, c0 + j), rows, stride=pitch), :] for j in range(BLOCK)], axis=0)
                    sh[s, k, pl.ds(0, BLOCK * rows), :] = v.astype(BF16)
                    for j in range(ring):
                        sc[s, k, pl.ds(j * rows, rows), :] = cm[pl.ds(ring * cols + cc0 + j, rows, stride=cols), :]
                else:
                    for i in range(BLOCK):
                        sq[s, k - 4, pl.ds(i * BLOCK, BLOCK), :] = hb[pl.ds(h_addr(r0 + i, c0), BLOCK), :]
                    for j in range(ring):
                        sq[s, k - 4, pl.ds(BLOCK * BLOCK + j * ring, ring), :] = cm[pl.ds((rc0 + ring) * cols + cc0 + j, ring, stride=cols), :]

        def unpack(s, par):
            hb = hbs[s][0]
            cm = cms[s]
            cs = css[s]
            for k in range(8):
                dr, dc = DIRS[k]
                o = opposite(k)
                r0 = -BLOCK if dr < 0 else rows
                c0 = -BLOCK if dc < 0 else cols
                st0 = 0 if dc < 0 else ring
                q0 = 0 if dr < 0 else rows + ring
                if dc == 0:
                    v = rh[par, s, o, pl.ds(0, BLOCK * cols), :].astype(F32)
                    for i in range(BLOCK):
                        hb[pl.ds(h_addr(r0 + i, 0), cols), :] = v[i * cols:(i + 1) * cols]
                    cm[pl.ds(q0 * cols, ring * cols), :] = rc[par, s, o]
                elif dr == 0:
                    v = rh[par, s, o, pl.ds(0, BLOCK * rows), :].astype(F32)
                    for j in range(BLOCK):
                        hb[pl.ds(h_addr(0, c0 + j), rows, stride=pitch), :] = v[j * rows:(j + 1) * rows]
                    for j in range(ring):
                        cs[pl.ds((st0 + j) * 32 + ring, rows), :] = rc[par, s, o, pl.ds(j * rows, rows), :]
                else:
                    for i in range(BLOCK):
                        hb[pl.ds(h_addr(r0 + i, c0), BLOCK), :] = rq[par, s, o - 4, pl.ds(i * BLOCK, BLOCK), :]
                    for j in range(ring):
                        cs[pl.ds((st0 + j) * 32 + q0, ring), :] = rq[par, s, o - 4, pl.ds(BLOCK * BLOCK + j * ring, ring), :]

        def send(s, dst):
            for k in (4, 5, 6, 7):
                msg_copies(s, k, dst)[0].start()
            for n in range(2):
                for k in (2, 3, 0, 1):
                    msg_copies(s, k, dst)[n].start()

        def wait_rows(sem, n):
            pltpu.make_async_copy(cinit.at[:, pl.ds(0, n // seqs)], cout.at[:, pl.ds(0, n // seqs)], sem).wait()

        def wait_all(sem, row_size, col_size, corner_size, absent=False, more=None):
            for a in ((1, 2) if row_count > 2 else (row_count - 1,)):
                for b in ((1, 2) if col_count > 2 else (col_count - 1,)):
                    n = row_size * a + col_size * b + corner_size * a * b
                    if absent:
                        n = 2 * row_size + 2 * col_size + 4 * corner_size - n
                    cond = jnp.logical_and((p_row if absent else n_row) == a, n_col == b)
                    if n:
                        @pl.when(cond if more is None else jnp.logical_and(cond, more))
                        def _():
                            wait_rows(sem, n)

        msg_side, msg_corner = 40 + ring * cols, 16
        msg_total = 4 * (msg_side + msg_corner)

        own_lane = xrow0 * chan
        row_lanes = rows * chan

        def x_copy(first, count, k, sem):
            dr, dc = DIRS[k]
            if dc == 0:
                per = BLOCK * seqs
                src = own_lane if dr < 0 else own_lane + row_lanes - 128
                dst = own_lane + row_lanes if dr < 0 else 0
                a = xt.at[pl.ds(first * per, count * per), pl.ds(COL0, cols), pl.ds(src, 128)]
                b = xt.at[pl.ds(first * per, count * per), pl.ds(COL0, cols), pl.ds(dst, 128)]
            else:
                width = row_lanes if dr == 0 else 128
                src = row_lanes - 128 if dr > 0 else 0
                dst = {-1: own_lane + row_lanes, 0: own_lane, 1: 0}[dr]
                a = xs.at[pl.ds(first, count), 0 if dc < 0 else 1, :, pl.ds(src, width)]
                b = xr.at[pl.ds(first, count), 1 if dc < 0 else 0, :, pl.ds(dst, width)]
            return pltpu.make_async_remote_copy(
                src_ref=a, dst_ref=b, send_sem=xssem.at[sem], recv_sem=xrsem.at[sem], device_id=dev(k), device_id_type=MESH)

        x_sizes = (BLOCK * seqs * cols, 16 * row_lanes // 256, 16 * 128 // 256)

        def x_rows_of(s, q):
            w = BLOCK - q
            return s * (BLOCK * (BLOCK + 1) // 2) + sum(BLOCK - p for p in range(q)), w

        def pack_x(blk):
            for side in range(2):
                for s in range(seqs):
                    for q in range(BLOCK):
                        at, w = x_rows_of(s, q)
                        col = COL0 if side == 0 else COL0 + cols - w
                        xtmp[side, pl.ds(at, w), :] = xt[(blk * BLOCK + q) * seqs + s, pl.ds(col, w), pl.ds(own_lane, row_lanes)]
                xs[blk, side] = xtmp[side].astype(BF16)

        def unpack_x(blk):
            for side in range(2):
                v = xr[blk, side].astype(F32)
                xtmp2[side] = v
                for s in range(seqs):
                    for q in range(BLOCK):
                        at, w = x_rows_of(s, q)
                        col = COL0 - w if side == 0 else COL0 + cols
                        xt[(blk * BLOCK + q) * seqs + s, pl.ds(col, w), :] = xtmp2[side, pl.ds(at, w), :]

        def load_state(s):
            for r in range(0, rows, 2):
                v = hin[s, pl.ds(r * cols, 2 * cols), :].astype(F32)
                for i in range(2):
                    hbs[s][0][pl.ds(h_addr(r + i, 0), cols), :] = v[i * cols:(i + 1) * cols]

        cp_h.wait()
        load_state(0)
        cp_c[0].wait()
        pack(0)

        eye = (lax.broadcasted_iota(jnp.int32, (cols, cols), 0) == lax.broadcasted_iota(jnp.int32, (cols, cols), 1)).astype(F32).astype(BF16)

        def prep_x(dst):
            for q in range(BLOCK):
                t = dst * BLOCK + q
                for s in range(seqs):
                    xt[t * seqs + s, pl.ds(COL0, cols), pl.ds(own_lane, row_lanes)] = lax.dot_general(
                        eye, fbuf[t * seqs + s], (((1,), (1,)), ((), ())), preferred_element_type=F32)


        cp_f.wait()
        prep_x(0)
        pack_x(0)
        met = (n_row + 1) * (n_col + 1) - 1
        pl.semaphore_wait(barrier, met + 8 - ((p_row + 1) * (n_col + 1) - 1))

        send(0, 0)

        def send_x(first, count, sem):
            for k in range(8):
                @pl.when(present[k])
                def _():
                    x_copy(first, count, k, sem).start()

        send_x(0, 1, 0)
        load_state(1)
        cp_c[1].wait()
        pack(1)
        send(1, 0)
        cp_w.wait()
        for cp in cp_small:
            cp.wait()
        wall[pl.ds(9 * hid, 3 * 128), :] = jnp.zeros((3 * 128, gates), BF16)
        for dc in range(3):
            for dr in range(3):
                wall[pl.ds(9 * hid + dc * 128 + dr * chan, chan), :] = wx_ref[dr, dc]

        cp_g.wait()

        def prep_more(blk, _):
            prep_x(blk)
            pack_x(blk)
            return 0

        lax.fori_loop(1, nblock, prep_more, 0)
        send_x(1, nblock - 1, 1)
        for k in range(8):
            o = opposite(k)

            @pl.when(jnp.logical_not(present[k]))
            def _():
                for par in range(2):
                    for s in range(seqs):
                        if k < 4:
                            rh[par, s, o] = jnp.zeros(rh.shape[3:], BF16)
                            rc[par, s, o] = jnp.zeros(rc.shape[3:], F32)
                        else:
                            rq[par, s, o - 4] = jnp.zeros(rq.shape[3:], F32)
                dr, dc = DIRS[k]
                if dc == 0:
                    lane0 = 0 if dr < 0 else own_lane + row_lanes

                    def zero_x(i, _):
                        xt[i, pl.ds(COL0, cols), pl.ds(lane0, 128)] = jnp.zeros((cols, 128), F32)
                        return 0

                    lax.fori_loop(0, steps * seqs, zero_x, 0)
                else:
                    lane0 = {-1: 0, 0: own_lane, 1: own_lane + row_lanes}[dr]
                    n = row_lanes if dr == 0 else 128
                    xr[:, 0 if dc < 0 else 1, :, pl.ds(lane0, n)] = jnp.zeros((nblock, 16, n), BF16)

        wait_all(xrsem.at[0], *x_sizes)
        unpack_x(0)
        lane = lax.broadcasted_iota(jnp.int32, (pitch, 128), 1)

        def build_xg(s, t, ext):
            xg = xgs[s]
            for r in range(-ext, rows + ext):
                start = r - 1 + xrow0
                g, off = divmod(start, 8)
                v = xt[t * seqs + s, :, pl.ds(g * 128, 128)]
                if off:
                    v = pltpu.roll(v, 128 - chan * off, 1)
                    if off > 5:
                        w = pltpu.roll(xt[t * seqs + s, :, pl.ds((g + 1) * 128, 128)], 128 - chan * off, 1)
                        v = jnp.where(lane < 128 - chan * off, v, w)
                xg[pl.ds(x_addr(r, -COL0), pitch), :] = v

        def build_lhs(s, j, ch, taps=tuple(range(12))):
            hb = hbs[s][j]
            xg = xgs[s]
            r0, nr, strips = chunk_list(BLOCK - 1 - j)[ch]
            lhs = lhss[ch]
            base = 32 * len(strips)
            for tap in taps:
                for n, k in enumerate(strips):
                    if tap < 9:
                        dr, dc = tap // 3 - 1, tap % 3 - 1
                        v = hb[pl.ds(h_addr(-ring + dr, strip_cols[k] + dc), 32, stride=pitch), :]
                    else:
                        v = xg[pl.ds(x_addr(-ring, strip_cols[k] + tap - 10), 32, stride=pitch), :]
                    lhs[pl.ds(32 * n, 32), pl.ds(tap * 128, 128)] = v.astype(BF16)

            def rows_of(ref, addr, r, cnt, dc):
                v = [ref[pl.ds(addr(r + i, dc), cols), :] for i in range(cnt)]
                return (jnp.concatenate(v, axis=0) if cnt > 1 else v[0]).astype(BF16)

            def put(tap, i, cnt, v):
                lhs[pl.ds(base + i * cols, cnt * cols), pl.ds(tap * 128, 128)] = v

            pairs = [(i, min(2, nr - i)) for i in range(0, nr, 2)]
            for dc in (-1, 0, 1):
                if dc + 10 in taps:
                    for i, cnt in pairs:
                        put(dc + 10, i, cnt, rows_of(xg, x_addr, r0 + i, cnt, dc))
                if dc + 1 in taps:
                    for i, cnt in pairs:
                        put(dc + 4, i, cnt, rows_of(hb, h_addr, r0 + i, cnt, dc))
                        if cnt == 2:
                            v = rows_of(hb, h_addr, r0 + i - 1, 2, dc)
                            put(dc + 1, i, 2, v)
                            if i:
                                put(dc + 7, i - 2, 2, v)
                        else:
                            v = rows_of(hb, h_addr, r0 + i - 1, 2, dc)
                            put(dc + 7, i - 2, 2, v)
                            put(dc + 1, i, 1, rows_of(hb, h_addr, r0 + i - 1, 1, dc))
                    i, cnt = pairs[-1]
                    put(dc + 7, i, cnt, rows_of(hb, h_addr, r0 + i + 1, cnt, dc))

        def matmul(j, ch):
            r0, nr, strips = chunk_list(BLOCK - 1 - j)[ch]
            m = -(-(32 * len(strips) + nr * cols) // 16) * 16
            gss[ch][pl.ds(0, m), :] = jnp.dot(lhss[ch][pl.ds(0, m), :], wall[...], preferred_element_type=F32)

        def cell(g_ref, m0, n, c):
            b = bias_ref[...]
            acts = []
            for q in range(4):
                g = g_ref[pl.ds(m0, n), pl.ds(q * hid, hid)] + b[:, q * hid:(q + 1) * hid]
                acts.append(jnp.tanh(g) if q == 3 else 0.5 * jnp.tanh(0.5 * g) + 0.5)
            c_new = acts[1] * c + acts[0] * acts[3]
            return acts[2] * jnp.tanh(c_new), c_new

        def elementwise(s, j, ch, t):
            ext = BLOCK - 1 - j
            dst = hbs[s][(j + 1) % BLOCK]
            r0, nr, strips = chunk_list(ext)[ch]
            base = 32 * len(strips)
            for n, k in enumerate(strips):
                h, c_new = cell(gss[ch], 32 * n, 32, css[s][pl.ds(32 * k, 32), :])
                css[s][pl.ds(32 * k, 32), :] = c_new
                h = h * smask[0 if strip_cols[k] < 0 else 1]
                dst[pl.ds(h_addr(-ring, strip_cols[k]), 32, stride=pitch), :] = h.astype(BF16).astype(F32)
            r = r0
            while r < r0 + nr:
                inside = 0 <= r < rows
                cnt = 2 if inside else 1
                crow = (r + ring) * cols
                c_old = cms[s][pl.ds(crow, cnt * cols), :]
                h, c_new = cell(gss[ch], base + (r - r0) * cols, cnt * cols, c_old)
                cms[s][pl.ds(crow, cnt * cols), :] = c_new
                if not inside:
                    h = h * (top_ok if r < 0 else bot_ok)
                hb16 = h.astype(BF16)
                if inside:
                    hout[t, s, pl.ds(r * cols, cnt * cols), :] = hb16
                h = hb16.astype(F32)
                for i in range(cnt):
                    dst[pl.ds(h_addr(r + i, 0), cols), :] = h[i * cols:(i + 1) * cols]
                r += cnt

        def block(b, _):
            par = lax.rem(b, 2)
            for s in range(seqs):
                o = 1 - s
                wait_all(rsem.at[par * seqs + s], msg_side, msg_side, msg_corner)
                wait_rows(ssem.at[s], msg_total)
                if s > 0:
                    wait_all(xrsem.at[1], *[(nblock - 1) * n for n in x_sizes], more=b == 0)
                unpack(s, par)
                build_lhs(s, 0, 0, tuple(range(9)))
                late = None
                for j in range(BLOCK):
                    if j > 0:
                        build_xg(s, b * BLOCK + j, BLOCK - 1 - j)
                    if s == seqs - 1 and j == BLOCK - 1:
                        unpack_x(lax.rem(b + 1, nblock))
                    for ch in range(3):
                        if j + ch > 0:
                            build_lhs(s, j, ch)
                        matmul(j, ch)
                        if late is not None:
                            elementwise(s, *late, b * BLOCK + late[0])
                        late = (j, ch)
                    if j == BLOCK - 1:
                        build_xg(o, lax.rem((b + s) * BLOCK, steps), BLOCK - 1)
                        build_lhs(o, 0, 0, (9, 10, 11))
                elementwise(s, *late, b * BLOCK + late[0])

                @pl.when(b < nblock - 1)
                def _():
                    pack(s)
                    send(s, b + 1)
            return 0

        build_xg(0, 0, BLOCK - 1)
        build_lhs(0, 0, 0, (9, 10, 11))
        lax.fori_loop(0, nblock, block, 0)
        wait_all(xssem.at[0], *x_sizes)
        wait_all(xssem.at[1], *[(nblock - 1) * n for n in x_sizes])
        for dst in range(nblock):
            for s in range(seqs):
                wait_all(rsem.at[(2 + dst) * seqs + s], msg_side, msg_side, msg_corner, absent=True)
        for s in range(seqs):
            cout[s] = cms[s][pl.ds(ring * cols, rows * cols), :]

    hbuf = pltpu.VMEM((hrows * pitch, hid), F32)
    xbuf = pltpu.VMEM((hrows * pitch, 128), F32)
    mmax = [-(-max(32 * len(chunk_list(e)[ch][2]) + chunk_list(e)[ch][1] * cols for e in range(BLOCK)) // 16) * 16 for ch in range(3)]
    scratch = (
        [hbuf] * 6 + [xbuf] * 2
        + [pltpu.VMEM(((rows + 2 * ring) * cols, hid), F32)] * 2
        + [pltpu.VMEM((nstrip * 32, hid), F32)] * 2
        + [
            pltpu.VMEM((steps * seqs, pitch, (rows + 16) * chan), F32),
            pltpu.VMEM((steps * seqs, rows * chan, cols), BF16),
            pltpu.VMEM((kdim, gates), BF16),
        ]
        + [pltpu.VMEM((mmax[ch], kdim), BF16) for ch in range(3)]
        + [pltpu.VMEM((mmax[ch], gates), F32) for ch in range(3)]
        + [
            pltpu.VMEM((3, 3, chan, gates), BF16),
            pltpu.VMEM((1, gates), F32),
            pltpu.VMEM((seqs, rows * cols, hid), BF16),
            pltpu.VMEM((seqs, 4, 80, hid), BF16),
            pltpu.VMEM((seqs, 4, ring * cols, hid), F32),
            pltpu.VMEM((seqs, 4, 16, hid), F32),
            pltpu.VMEM((2 + nblock, seqs, 4, 80, hid), BF16),
            pltpu.VMEM((2 + nblock, seqs, 4, ring * cols, hid), F32),
            pltpu.VMEM((2 + nblock, seqs, 4, 16, hid), F32),
            pltpu.VMEM((nblock, 2, 16, rows * chan), BF16),
            pltpu.VMEM((nblock, 2, 16, (rows + 16) * chan), BF16),
            pltpu.VMEM((2, 16, rows * chan), F32),
            pltpu.VMEM((2, 16, (rows + 16) * chan), F32),
            pltpu.VMEM((2, 32, hid), F32),
            pltpu.SemaphoreType.DMA((8,)),
            pltpu.SemaphoreType.DMA((seqs,)),
            pltpu.SemaphoreType.DMA(((2 + nblock) * seqs,)),
            pltpu.SemaphoreType.DMA((2,)),
            pltpu.SemaphoreType.DMA((2,)),
        ]
    )
    return kernel, scratch


def solution(mesh):
    row_count = mesh.shape["rows"]
    col_count = mesh.shape["cols"]
    frame_spec = P(None, "batch", "rows", "cols", None)
    state_spec = P("batch", "rows", "cols", None)

    def local_run(frames, w_x, w_h, gate_bias, h_init, c_init):
        steps, seqs, rows, cols, chan = frames.shape
        hid = h_init.shape[-1]
        gates = 4 * hid
        kernel, scratch = make_kernel(steps, seqs, rows, cols, chan, hid, row_count, col_count)
        hbm = pl.BlockSpec(memory_space=pltpu.HBM)
        vmem = pl.BlockSpec(memory_space=pltpu.VMEM)
        ft = frames.transpose(0, 1, 2, 4, 3).reshape(steps * seqs, rows * chan, cols)
        all_hidden, cell_last = pl.pallas_call(
            kernel,
            out_shape=(
                pltpu.VMEM((steps, seqs, rows * cols, hid), BF16),
                pltpu.VMEM((seqs, rows * cols, hid), F32),
            ),
            in_specs=[hbm] * 6,
            out_specs=(vmem, vmem),
            scratch_shapes=scratch,
            compiler_params=pltpu.CompilerParams(collective_id=0, has_side_effects=True, vmem_limit_bytes=44 * 1024 * 1024),
        )(
            *[
                pltpu.with_memory_space_constraint(x, pltpu.HBM)
                for x in (
                    ft, w_x, w_h.reshape(9 * hid, gates), gate_bias.reshape(1, gates),
                    h_init.reshape(seqs, rows * cols, hid), c_init.reshape(seqs, rows * cols, hid),
                )
            ]
        )
        return all_hidden.reshape(steps, seqs, rows, cols, hid), cell_last.reshape(seqs, rows, cols, hid)

    return jax.shard_map(local_run, mesh=mesh, in_specs=(frame_spec, P(), P(), P(), state_spec, state_spec), out_specs=(frame_spec, state_spec), check_vma=False)
```
